256 devices in a mesh: ent: 128 (over x, y, z_lo, core), grp: 2 (over z_hi).
Axes of the slice: x: 4, y: 4, z: 8 (z_hi: 2, z_lo: 4; z = z_hi * 4 + z_lo), core: 2. Of those that a mesh axis runs over, the one named last changes fastest.
Arguments:
- entity_table: bfloat16 [65536, 1024], P('ent'), may hold values from -2.5 to 2.5
- rel_phases: float32 [822, 512], replicated, may hold values from -3.1416 to 3.1416
- head_ids: int32 [65536], P(('ent', 'grp')), may hold values from 0 to 511
- rel_ids: int32 [65536], P(('ent', 'grp')), may hold values from 0 to 821
- target_pos: int32 [65536], P(('ent', 'grp')), may hold values from 0 to 511
- block_owner: int32 [4], replicated, may hold values from 0 to 127
- block_local: int32 [4], replicated, may hold values from 0 to 3
Outputs:
- losses: float32 [65536], P(('ent', 'grp'))
- head_grad: bfloat16 [65536, 1024], P(('ent', 'grp'))
- table_grad: bfloat16 [65536, 1024], P('ent')
- rel_grad: float32 [822, 512], replicated
The draws below stay inside these ranges and needn't reach their ends.
Inputs may be any that keep to these rules, and one draw needn't show every extreme that they name: query q on device d (ent then grp) has head row (d // 2) * 512 + head_ids[q]. `target_pos`: position among the 512 candidates, block after block. Block b covers table rows from (block_owner[b] * 4 + block_local[b]) * 128 on; blocks may repeat.
All inputs are finite; a program needn't handle non-finite values.
Results may differ from the reference program's by a relative error of at most 0.0057.
Values may be sent and summed in bfloat16 or wider, within the bound.
No kernel may reach another device: no remote copies, remote signals or barrier semaphores. Data moves between devices by JAX's collectives and lax.ppermute only.
A program may use at most 64 MiB of HBM per device.

```python
import math
import jax
import jax.numpy as jnp
import numpy as np
from jax import lax

K = 512
R = 822
BLK = 128
NBLK = 4
ENT_DEV = 512
Q_DEV = 256
SHARDS = 128
NENT = 65536
QUERIES = 65536
CAND = 512
N_ENT = 128
N_GRP = 2


def draw_entity_table(key, part):
    key_noise = jax.random.fold_in(key, 2)
    values = jnp.clip(0.25 * jax.random.normal(key_noise, (NENT, 2 * K), jnp.float32), -1.5, 1.5)
    return values.astype(jnp.bfloat16)


def draw_rel_phases(key, part):
    return jax.random.uniform(key, (R, K), jnp.float32, -3.1415, 3.1415)


def plant(values, rng, least, high):
    longest = values.shape.index(max(values.shape))
    spots = []
    for shift in (0, 1):
        where = [jax.random.randint(jax.random.fold_in(rng, axis), (), 0, length) for axis, length in enumerate(values.shape)]
        where[longest] = (where[longest] + shift) % values.shape[longest]
        spots.append(tuple(where))
    return values.at[spots[0]].set(least).at[spots[1]].set(high)


def cumulative_ranks(amount, slope):
    portions = [(1 << 20) // math.isqrt(grade ** slope) + 1 for grade in range(1, amount + 1)]
    width = 1 + sum(portions) // (1 << 30)
    return np.cumsum(np.array([max(1, weight // width) for weight in portions]))


def ranked(key, extent, number_of, lean):
    listing = cumulative_ranks(number_of, lean)
    ticket = jax.random.randint(jax.random.fold_in(key, 1), extent, 0, int(listing[number_of - 1]))
    rank = jnp.searchsorted(jnp.asarray(listing, jnp.int32), ticket, side="right")
    return jax.random.permutation(jax.random.fold_in(key, 2), number_of)[rank].astype(jnp.int32)


def setup_inputs(seed: int = 0) -> dict:
    arg_keys = jax.random.split(jax.random.key(seed), 8)
    return {
        "entity_table": draw_entity_table(jax.random.fold_in(arg_keys[7], 71), 0),
        "rel_phases": draw_rel_phases(jax.random.fold_in(arg_keys[7], 71), 0),
        "head_ids": plant(jax.random.randint(arg_keys[2], (QUERIES,), 0, ENT_DEV), jax.random.fold_in(arg_keys[2], 1), 0, ENT_DEV - 1).astype(jnp.int32),
        "rel_ids": plant(ranked(arg_keys[3], (QUERIES,), R, 2), jax.random.fold_in(arg_keys[3], 3), 0, R - 1).astype(jnp.int32),
        "target_pos": plant(jax.random.randint(arg_keys[4], (QUERIES,), 0, CAND), jax.random.fold_in(arg_keys[4], 1), 0, CAND - 1).astype(jnp.int32),
        "block_owner": plant(jax.random.randint(arg_keys[5], (NBLK,), 0, SHARDS), jax.random.fold_in(arg_keys[5], 1), 0, SHARDS - 1).astype(jnp.int32),
        "block_local": plant(jax.random.randint(arg_keys[6], (NBLK,), 0, ENT_DEV // BLK), jax.random.fold_in(arg_keys[6], 1), 0, (ENT_DEV // BLK) - 1).astype(jnp.int32),
    }


SOFTMAX_TEMPER = 2.0


def device_terms(heads, angles, targets, candidate_block, candidate_norm):
    half_dim = angles.shape[1]
    real_head = heads[:, :half_dim]
    imag_head = heads[:, half_dim:]
    cosine = jnp.cos(angles)
    sine = jnp.sin(angles)
    real_query = real_head * cosine - imag_head * sine
    imag_query = real_head * sine + imag_head * cosine
    query_reduced_precision = jnp.concatenate([real_query, imag_query], axis=1).astype(jnp.bfloat16)
    query_reduced_precision = lax.optimization_barrier(query_reduced_precision).astype(jnp.float32)
    logit_scores = (2.0 * jnp.dot(query_reduced_precision, candidate_block.T, precision=lax.Precision.HIGHEST) - candidate_norm[None, :]) / SOFTMAX_TEMPER
    top = jnp.max(logit_scores, axis=1, keepdims=True)
    log_total = top[:, 0] + jnp.log(jnp.sum(jnp.exp(logit_scores - top), axis=1))
    picked = jnp.take_along_axis(logit_scores, targets[:, None], axis=1)[:, 0]
    losses = log_total - picked
    columns = jnp.arange(logit_scores.shape[1], dtype=jnp.int32)
    onehot = (columns[None, :] == targets[:, None]).astype(jnp.float32)
    softmax_weights = jnp.exp(logit_scores - log_total[:, None]) - onehot
    weights_reduced_precision = lax.optimization_barrier(softmax_weights.astype(jnp.bfloat16)).astype(jnp.float32)
    query_gradient = (2.0 / SOFTMAX_TEMPER) * jnp.dot(weights_reduced_precision, candidate_block, precision=lax.Precision.HIGHEST)
    candidate_gradient = (2.0 / SOFTMAX_TEMPER) * (jnp.dot(weights_reduced_precision.T, query_reduced_precision, precision=lax.Precision.HIGHEST) - jnp.sum(softmax_weights, axis=0)[:, None] * candidate_block)
    real_grad = query_gradient[:, :half_dim]
    imag_grad = query_gradient[:, half_dim:]
    head_grad = jnp.concatenate([real_grad * cosine + imag_grad * sine, imag_grad * cosine - real_grad * sine], axis=1).astype(jnp.bfloat16)
    angle_grad = imag_grad * real_query - real_grad * imag_query
    return losses, head_grad, angle_grad, candidate_gradient


def reference(entity_table, rel_phases, head_ids, rel_ids, target_pos, block_owner, block_local):
    half_dim = rel_phases.shape[1]
    rel_count = rel_phases.shape[0]
    devices = N_ENT * N_GRP
    starts = (block_owner * (ENT_DEV // BLK) + block_local) * BLK
    rows = (starts[:, None] + jnp.arange(BLK, dtype=jnp.int32)[None, :]).reshape(-1).astype(jnp.int32)
    candidate_block = entity_table[rows].astype(jnp.float32)
    candidate_norm = jnp.sum(candidate_block * candidate_block, axis=1)

    def step(carry, inputs):
        cand_total, rel_total = carry
        head_local, rel_local, target_local, device = inputs
        head_rows = ((device // N_GRP) * ENT_DEV + head_local).astype(jnp.int32)
        heads = entity_table[head_rows].astype(jnp.float32)
        angles = rel_phases[rel_local]
        losses, head_grad, angle_grad, candidate_gradient = device_terms(heads, angles, target_local, candidate_block, candidate_norm)
        rel_part = jax.ops.segment_sum(angle_grad, rel_local, num_segments=rel_count)
        return (cand_total + candidate_gradient, rel_total + rel_part), (losses, head_grad)

    start_carry = (jnp.zeros((NBLK * BLK, 2 * half_dim), jnp.float32), jnp.zeros((rel_count, half_dim), jnp.float32))
    inputs = (head_ids.reshape(devices, Q_DEV), rel_ids.reshape(devices, Q_DEV), target_pos.reshape(devices, Q_DEV), jnp.arange(devices, dtype=jnp.int32))
    (cand_total, rel_grad), (losses, head_grad) = lax.scan(step, start_carry, inputs)
    table_grad = jax.ops.segment_sum(cand_total, rows, num_segments=NENT).astype(jnp.bfloat16)
    return losses.reshape(-1), head_grad.reshape(-1, 2 * half_dim), table_grad, rel_grad
```

```python
import jax
import jax.numpy as jnp
from jax import lax
from jax.experimental import pallas as pl
from jax.experimental.pallas import tpu as pltpu
from jax.sharding import Mesh
from jax.sharding import PartitionSpec as P

BLK = 128
ENT = ("x", "y", "zl", "core")
ENT_GRP = ("x", "y", "zl", "core", "grp")
PLANE = ("x", "y")
LINE = ("zl", "grp")
SWAP = [(0, 1), (1, 0)]
BF = jnp.bfloat16
F32 = jnp.float32
NT = (((1,), (1,)), ((), ()))
TN = (((0,), (0,)), ((), ()))
VMEM = pl.BlockSpec(memory_space=pltpu.VMEM)
SMEM = pl.BlockSpec(memory_space=pltpu.SMEM)
RELS = 64
LIMIT = 60 * 1024 * 1024


def dot(a, b, dims=(((1,), (0,)), ((), ()))):
    return lax.dot_general(a, b, dims, preferred_element_type=F32)


def split_sum(ones, x, dims, ones_first):
    hi = x.astype(BF)
    lo = (x - hi.astype(F32)).astype(BF)
    if ones_first:
        return dot(ones, hi, dims) + dot(ones, lo, dims)
    return dot(hi, ones, dims) + dot(lo, ones, dims)


def main_kernel(
    core_ref, heads_ref, query_ref, own_ref, other_ref, target_ref, cos_ref, sin_ref,
    loss_ref, head_ref, keep_ref, send_ref, ang_keep_ref, ang_send_ref,
):
    rows, half = cos_ref.shape
    n = own_ref.shape[0]
    query = query_ref[...]
    cands = (own_ref[...], other_ref[...])
    target = jnp.broadcast_to(target_ref[...], (128, rows)).T[:, :1]
    ones8 = jnp.ones((8, 2 * half), BF)
    scores = []
    for cand in cands:
        wide = cand.astype(F32)
        norm = split_sum(ones8, wide * wide, NT, True)[:1]
        scores.append(dot(query, cand, NT) - 0.5 * norm)
    top = jnp.maximum(
        jnp.max(scores[0], axis=1, keepdims=True), jnp.max(scores[1], axis=1, keepdims=True)
    )
    exps = [jnp.exp(s - top) for s in scores]
    total = jnp.sum(exps[0], axis=1, keepdims=True) + jnp.sum(exps[1], axis=1, keepdims=True)
    lanes = lax.broadcasted_iota(jnp.int32, (rows, n), 1)
    hits = [lanes == target, lanes + n == target]
    picked = sum(jnp.sum(jnp.where(h, s, 0.0), axis=1, keepdims=True) for h, s in zip(hits, scores))
    loss = top + jnp.log(total) - picked
    loss_ref[...] = jnp.broadcast_to(loss, (rows, 128)).T[:1]
    scale = 1.0 / total
    ones_q = jnp.ones((rows, 128), BF)
    dquery = None
    for k in range(2):
        weights = exps[k] * scale - hits[k].astype(F32)
        low = weights.astype(BF)
        part = dot(low, cands[k])
        dquery = part if dquery is None else dquery + part
        column = split_sum(ones_q, weights, TN, False)[:, :1]
        grad = dot(low, query, TN) - column * cands[k].astype(F32)
        if k == 0:
            keep_ref[...] = grad
        else:
            send_ref[...] = grad.astype(BF)
    cosine = cos_ref[...]
    sine = sin_ref[...]
    heads = heads_ref[...].astype(F32)
    hr, hi = heads[:, :half], heads[:, half:]
    qr = hr * cosine - hi * sine
    qi = hr * sine + hi * cosine
    dr, di = dquery[:, :half], dquery[:, half:]
    head_ref[:, :half] = (dr * cosine + di * sine).astype(BF)
    head_ref[:, half:] = (di * cosine - dr * sine).astype(BF)
    ang = di * qr - dr * qi
    a, b = ang[:, : half // 2], ang[:, half // 2 :]
    first = core_ref[0] == 0
    ang_keep_ref[...] = jnp.where(first, a, b)
    ang_send_ref[...] = jnp.where(first, b, a)


def pack_kernel(ids_ref, keep_ref, got_ref, ang_ref, ang_got_ref, out_ref):
    pieces, piece_rows, width = out_ref.shape
    cand_rows = keep_ref.shape[0] // pieces
    grad = keep_ref[...] + got_ref[...].astype(F32)
    out_ref[:, :cand_rows, :] = grad.astype(BF).reshape(pieces, cand_rows, width)
    used = 13 * RELS
    rel = lax.broadcasted_iota(jnp.int32, (used, ids_ref.shape[1]), 0)
    pick = (rel == ids_ref[...]).astype(F32).astype(BF)
    q = ang_ref.shape[0]
    total = None
    for k, ref in enumerate((ang_ref, ang_got_ref)):
        x = ref[...]
        hi = x.astype(BF)
        lo = (x - hi.astype(F32)).astype(BF)
        sel = pick[:, k * q : (k + 1) * q]
        part = dot(sel, hi) + dot(sel, lo)
        total = part if total is None else total + part
    w = ang_ref.shape[1]
    total = total.astype(BF)
    rr = piece_rows - cand_rows
    for j in range(pieces):
        for k in range(width // w):
            if j < 13:
                at = j * RELS + k * rr
                out_ref[j, cand_rows:, k * w : (k + 1) * w] = total[at : at + rr]
            else:
                out_ref[j, cand_rows:, k * w : (k + 1) * w] = jnp.zeros((rr, w), BF)


def place_kernel(core_ref, me_ref, owner_ref, local_ref, own_ref, other_ref, table_ref, rel_ref):
    pieces, piece_rows, width = own_ref.shape
    cand_rows = piece_rows // 2
    rels, rel_width = rel_ref.shape
    w = rel_width // 2
    table_ref[...] = jnp.zeros_like(table_ref)
    core = core_ref[0]
    for b in range(4):
        g, h = b // 2, b % 2

        @pl.when(owner_ref[b] == me_ref[0])
        def _():
            start = pl.multiple_of(local_ref[b] * BLK, BLK)
            for j in range(pieces):
                at = pl.ds(start + j * 8, 8)
                lo, hi = g * 8, g * 8 + 8
                block = jnp.where(
                    core == h,
                    own_ref[j, lo:hi, :].astype(F32),
                    other_ref[j, lo:hi, :].astype(F32),
                )
                table_ref[at, :] = (table_ref[at, :].astype(F32) + block).astype(BF)

    rr = piece_rows - cand_rows
    for h in range(2):
        for j in range(pieces):
            for k in range(width // w):
                at = j * RELS + k * rr
                size = min(rr, rels - at)
                if size > 0:
                    cols = slice(k * w, (k + 1) * w)
                    rel_ref[at : at + size, h * w : (h + 1) * w] = jnp.where(
                        core == h,
                        own_ref[j, cand_rows : cand_rows + size, cols].astype(F32),
                        other_ref[j, cand_rows : cand_rows + size, cols].astype(F32),
                    )


def exchange(x, axes):
    return lax.all_to_all(x, axes, split_axis=0, concat_axis=0, tiled=True)


def copies(x, n):
    return jnp.broadcast_to(x[None], (n, *x.shape))


def body(entity_table, rel_phases, head_ids, rel_ids, target_pos, block_owner, block_local):
    half = rel_phases.shape[1]
    rels = rel_phases.shape[0]
    width = 2 * half
    queries = head_ids.shape[0]
    core = lax.axis_index("core")
    grp = lax.axis_index("grp")
    me = lax.axis_index(ENT)
    plane = lax.axis_size(PLANE)
    line = lax.axis_size(LINE)
    rows = BLK // plane

    def mine(b):
        block = lax.dynamic_slice_in_dim(entity_table, block_local[b] * BLK, BLK, 0)
        return jnp.where(block_owner[b] == me, block, jnp.zeros_like(block))

    ids_other = lax.ppermute(rel_ids, "core", SWAP)
    kept = mine(2 * grp + core)
    passed = lax.ppermute(mine(2 * grp + 1 - core), "core", SWAP)
    block = (kept + passed).reshape(plane, rows, width)
    piece = jnp.sum(exchange(block, PLANE).astype(F32), axis=0).astype(BF)
    pieces = exchange(copies(piece, line), LINE).reshape(line // 2, 2, rows, width)
    piece = jnp.sum(pieces.astype(F32), axis=0).astype(BF).reshape(2 * rows, width)
    own = exchange(copies(piece, plane), PLANE).reshape(2 * BLK, width)
    other = lax.ppermute(own, "core", SWAP)

    heads = jnp.take(entity_table, head_ids, axis=0)
    angles = jnp.take(rel_phases, rel_ids, axis=0)
    cosine = jnp.cos(angles)
    sine = jnp.sin(angles)
    wide = heads.astype(F32)
    hr, hi = wide[:, :half], wide[:, half:]
    query = jnp.concatenate([hr * cosine - hi * sine, hr * sine + hi * cosine], axis=1).astype(BF)
    b, t = target_pos // BLK, target_pos % BLK
    place = ((b % 2) ^ core) * (2 * BLK) + (t // rows) * (2 * rows) + (b // 2) * rows + t % rows
    core_at = core.astype(jnp.int32).reshape(1)

    n = 2 * BLK
    loss, head_grad, keep, send, ang_keep, ang_send = pl.pallas_call(
        main_kernel,
        out_shape=(
            jax.ShapeDtypeStruct((1, queries), F32),
            jax.ShapeDtypeStruct((queries, width), BF),
            jax.ShapeDtypeStruct((n, width), F32),
            jax.ShapeDtypeStruct((n, width), BF),
            jax.ShapeDtypeStruct((queries, half // 2), F32),
            jax.ShapeDtypeStruct((queries, half // 2), F32),
        ),
        in_specs=[SMEM] + [VMEM] * 7,
        out_specs=(VMEM,) * 6,
        compiler_params=pltpu.CompilerParams(vmem_limit_bytes=LIMIT),
        cost_estimate=pl.CostEstimate(
            flops=6 * queries * 2 * n * width, bytes_accessed=6_000_000, transcendentals=queries * n
        ),
        name="main_kernel",
    )(core_at, heads, query, own, other, place.reshape(1, queries), cosine, sine)

    got = lax.ppermute(send, "core", SWAP)
    ang_got = lax.ppermute(ang_send, "core", SWAP)
    ids = jnp.concatenate([rel_ids, ids_other]).reshape(1, 2 * queries)
    packed = pl.pallas_call(
        pack_kernel,
        out_shape=jax.ShapeDtypeStruct((plane, 4 * rows, width), BF),
        in_specs=[VMEM] * 5,
        out_specs=VMEM,
        compiler_params=pltpu.CompilerParams(vmem_limit_bytes=LIMIT),
        cost_estimate=pl.CostEstimate(
            flops=4 * queries * 1024 * half, bytes_accessed=4_000_000, transcendentals=0
        ),
        name="pack_kernel",
    )(ids, keep, got, ang_keep, ang_got)
    part = jnp.sum(exchange(packed, PLANE).astype(F32), axis=0).astype(BF)
    part = jnp.sum(exchange(copies(part, line), LINE).astype(F32), axis=0).astype(BF)
    own_sum = exchange(copies(part, plane), PLANE)
    other_sum = lax.ppermute(own_sum, "core", SWAP)
    table_grad, rel_grad = pl.pallas_call(
        place_kernel,
        out_shape=(
            jax.ShapeDtypeStruct(entity_table.shape, BF),
            jax.ShapeDtypeStruct((rels, half), F32),
        ),
        in_specs=[SMEM] * 4 + [VMEM] * 2,
        out_specs=(VMEM, VMEM),
        compiler_params=pltpu.CompilerParams(vmem_limit_bytes=LIMIT),
        cost_estimate=pl.CostEstimate(flops=1_000_000, bytes_accessed=5_000_000, transcendentals=0),
        name="place_kernel",
    )(core_at, me.astype(jnp.int32).reshape(1), block_owner, block_local, own_sum, other_sum)
    return loss.reshape(queries), head_grad, table_grad, rel_grad


def solution(mesh):
    finer = Mesh(
        mesh.devices.reshape(4, 4, 4, 2, mesh.shape["grp"]),
        ENT_GRP,
    )
    placed = (P(ENT, None), P(), P(ENT_GRP), P(ENT_GRP), P(ENT_GRP), P(), P())
    return jax.shard_map(
        body,
        mesh=finer,
        in_specs=placed,
        out_specs=(P(ENT_GRP), P(ENT_GRP, None), P(ENT, None), P()),
        check_vma=False,
    )
```

```python
import jax
import jax.numpy as jnp
from jax import lax
from jax.experimental import pallas as pl
from jax.experimental.pallas import tpu as pltpu
from jax.sharding import Mesh
from jax.sharding import PartitionSpec as P


BLK = 128
LANES = 128
ENT = ("x", "y", "zl", "core")
ENT_GRP = ("x", "y", "zl", "core", "grp")
PLANE = ("x", "y")
LINE = ("zl", "grp")
SWAP = [(0, 1), (1, 0)]
BF = jnp.bfloat16
F32 = jnp.float32
NT = (((1,), (1,)), ((), ()))
TN = (((0,), (0,)), ((), ()))
VMEM = pl.BlockSpec(memory_space=pltpu.VMEM)
SMEM = pl.BlockSpec(memory_space=pltpu.SMEM)
HBM = pl.BlockSpec(memory_space=pltpu.HBM)
MIB = 1024 * 1024


def dot(a, b, dims=(((1,), (0,)), ((), ()))):
    return lax.dot_general(a, b, dims, preferred_element_type=F32)


def halves(x):
    hi = x.astype(BF)
    return hi, (x - hi.astype(F32)).astype(BF)


def own_shard():
    place = lax.axis_index(ENT[0])
    for axis in ENT[1:]:
        place = place * lax.axis_size(axis) + lax.axis_index(axis)
    return place


def fetch_kernel(owner_ref, local_ref, table_ref, keep_ref, pass_ref, sem):
    core = lax.axis_index("core")
    grp = lax.axis_index("grp")
    me = own_shard()
    for b, out_ref in ((2 * grp + core, keep_ref), (2 * grp + 1 - core, pass_ref)):

        @pl.when(owner_ref[b] == me)
        def _():
            start = pl.multiple_of(local_ref[b] * BLK, BLK)
            copy = pltpu.make_async_copy(table_ref.at[pl.ds(start, BLK)], out_ref, sem)
            copy.start()
            copy.wait()

        @pl.when(owner_ref[b] != me)
        def _():
            out_ref[...] = jnp.zeros_like(out_ref)


def prep_kernel(
    heads_ref, angles_ref, target_ref, ids_ref, ids_other_ref,
    query_ref, cos_ref, sin_ref, spot_ref, pick_ref,
):
    half = cos_ref.shape[1]
    rows = query_ref.shape[0]
    angles = angles_ref[...]
    cosine = jnp.cos(angles)
    sine = jnp.sin(angles)
    cos_ref[...] = cosine
    sin_ref[...] = sine
    hr = heads_ref[:, :half].astype(F32)
    hi = heads_ref[:, half:].astype(F32)
    query_ref[:, :half] = (hr * cosine - hi * sine).astype(BF)
    query_ref[:, half:] = (hr * sine + hi * cosine).astype(BF)
    t = target_ref[...]
    core = lax.axis_index("core")
    block, row = t >> 7, t & 127
    spot = (((block & 1) ^ core) << 8) + ((row >> 3) << 4) + ((block >> 1) << 3) + (row & 7)
    spot_ref[...] = jnp.broadcast_to(spot, (LANES, rows)).T
    rel = lax.broadcasted_iota(jnp.int32, (pick_ref.shape[0], rows), 0)
    pick_ref[:, :rows] = (rel == ids_ref[...]).astype(F32).astype(BF)
    pick_ref[:, rows:] = (rel == ids_other_ref[...]).astype(F32).astype(BF)


def main_kernel(
    heads_ref, query_ref, own_ref, other_ref, spot_ref, cos_ref, sin_ref,
    loss_ref, head_ref, keep_ref, send_ref, ang_keep_ref, ang_send_ref,
):
    rows, half = cos_ref.shape
    n = own_ref.shape[0]
    query = query_ref[...]
    cands = (own_ref[...], other_ref[...])
    spot = spot_ref[:, :1]
    ones8 = jnp.ones((8, 2 * half), BF)
    scores = []
    for cand in cands:
        wide = cand.astype(F32)
        hi, lo = halves(wide * wide)
        norm = (dot(ones8, hi, NT) + dot(ones8, lo, NT))[:1]
        scores.append(dot(query, cand, NT) - 0.5 * norm)
    top = jnp.maximum(
        jnp.max(scores[0], axis=1, keepdims=True), jnp.max(scores[1], axis=1, keepdims=True)
    )
    exps = [jnp.exp(s - top) for s in scores]
    total = jnp.sum(exps[0], axis=1, keepdims=True) + jnp.sum(exps[1], axis=1, keepdims=True)
    lanes = lax.broadcasted_iota(jnp.int32, (rows, n), 1)
    hits = [lanes == spot, lanes + n == spot]
    picked = sum(jnp.sum(jnp.where(h, s, 0.0), axis=1, keepdims=True) for h, s in zip(hits, scores))
    loss = top + jnp.log(total) - picked
    loss_ref[...] = jnp.broadcast_to(loss, (rows, LANES)).T[:1]
    scale = 1.0 / total
    ones_q = jnp.ones((rows, LANES), BF)
    dquery = None
    for k in (1, 0):
        weights = exps[k] * scale - hits[k].astype(F32)
        low, rest = halves(weights)
        part = dot(low, cands[k])
        dquery = part if dquery is None else dquery + part
        column = (dot(low, ones_q, TN) + dot(rest, ones_q, TN))[:, :1]
        grad = dot(low, query, TN) - column * cands[k].astype(F32)
        if k == 0:
            keep_ref[...] = grad
        else:
            send_ref[...] = grad.astype(BF)
    cosine = cos_ref[...]
    sine = sin_ref[...]
    hr = heads_ref[:, :half].astype(F32)
    hi = heads_ref[:, half:].astype(F32)
    qr = hr * cosine - hi * sine
    qi = hr * sine + hi * cosine
    dr, di = dquery[:, :half], dquery[:, half:]
    head_ref[:, :half] = (dr * cosine + di * sine).astype(BF)
    head_ref[:, half:] = (di * cosine - dr * sine).astype(BF)
    ang = di * qr - dr * qi
    a, b = ang[:, : half // 2], ang[:, half // 2 :]
    first = lax.axis_index("core") == 0
    ang_keep_ref[...] = jnp.where(first, a, b)
    ang_send_ref[...] = jnp.where(first, b, a)


def pack_kernel(pick_ref, keep_ref, got_ref, ang_ref, ang_got_ref, out_ref):
    pieces = out_ref.shape[0]
    per = keep_ref.shape[0] // pieces
    groups = keep_ref.shape[1] // LANES
    for k in range(groups):
        cols = slice(k * LANES, (k + 1) * LANES)
        grad = keep_ref[:, cols] + got_ref[:, cols].astype(F32)
        out_ref[:, k * per : (k + 1) * per, :] = grad.astype(BF).reshape(pieces, per, LANES)
    q = ang_ref.shape[0]
    total = None
    for k, ref in enumerate((ang_ref, ang_got_ref)):
        sel = pick_ref[:, k * q : (k + 1) * q]
        hi, lo = halves(ref[...])
        part = dot(sel, hi) + dot(sel, lo)
        total = part if total is None else total + part
    total = total.astype(BF)
    base = groups * per
    size = out_ref.shape[1] - base
    row_groups = total.shape[0] // size
    for j in range(pieces):
        at = (j % row_groups) * size
        col = (j // row_groups) * LANES
        out_ref[j, base:, :] = total[at : at + size, col : col + LANES]


def place_kernel(owner_ref, local_ref, own_ref, other_ref, table_ref, rel_ref):
    pieces, piece_rows, _ = own_ref.shape
    groups = table_ref.shape[1] // LANES
    rels, rel_width = rel_ref.shape
    per = BLK // pieces
    table_ref[...] = jnp.zeros_like(table_ref)
    core = lax.axis_index("core")
    me = own_shard()
    for b in range(4):
        g, h = b // 2, b % 2

        def add(src_ref, g=g, b=b):
            start = pl.multiple_of(local_ref[b] * BLK, BLK)
            for k in range(groups):
                at = k * 2 * per + g * per
                block = src_ref[:, at : at + per, :].astype(F32).reshape(BLK, LANES)
                cols = slice(k * LANES, (k + 1) * LANES)
                old = table_ref[pl.ds(start, BLK), cols].astype(F32)
                table_ref[pl.ds(start, BLK), cols] = (old + block).astype(BF)

        mine = owner_ref[b] == me
        pl.when(mine & (core == h))(lambda add=add: add(own_ref))
        pl.when(mine & (core != h))(lambda add=add: add(other_ref))

    base = groups * 2 * per
    size = piece_rows - base
    row_groups = pieces * LANES * 2 // rel_width
    for h in range(2):

        def spread(src_ref, h=h):
            for j in range(pieces):
                at = (j % row_groups) * size
                rows = min(size, rels - at)
                col = h * (rel_width // 2) + (j // row_groups) * LANES
                rel_ref[at : at + rows, col : col + LANES] = src_ref[
                    j, base : base + rows, :
                ].astype(F32)

        pl.when(core == h)(lambda spread=spread: spread(own_ref))
        pl.when(core != h)(lambda spread=spread: spread(other_ref))


def exchange(x, axes):
    return lax.all_to_all(x, axes, split_axis=0, concat_axis=0, tiled=True)


def copies(x, n):
    return jnp.broadcast_to(x[None], (n, *x.shape))


def call(kernel, ins, specs, outs, grant, flops, nbytes, scratch=()):
    shapes = tuple(jax.ShapeDtypeStruct(s, d) for s, d in outs)
    single = len(shapes) == 1
    return pl.pallas_call(
        kernel,
        out_shape=shapes[0] if single else shapes,
        in_specs=specs,
        out_specs=VMEM if single else (VMEM,) * len(shapes),
        scratch_shapes=list(scratch),
        compiler_params=pltpu.CompilerParams(vmem_limit_bytes=grant),
        cost_estimate=pl.CostEstimate(flops=flops, bytes_accessed=nbytes, transcendentals=0),
    )(*ins)


def body(entity_table, rel_phases, head_ids, rel_ids, target_pos, block_owner, block_local):
    half = rel_phases.shape[1]
    rels = rel_phases.shape[0]
    width = 2 * half
    queries = head_ids.shape[0]
    plane = lax.axis_size(PLANE)
    line = lax.axis_size(LINE)
    rows = BLK // plane
    n = 2 * BLK
    rel_rows = -(-rels // 64) * 64
    piece_rows = n * width // (plane * LANES) + rel_rows * half // 2 // (plane * LANES)

    kept, passed = call(
        fetch_kernel, (block_owner, block_local, entity_table), [SMEM, SMEM, HBM],
        [((BLK, width), BF)] * 2, 2 * MIB, 100_000, 500_000, [pltpu.SemaphoreType.DMA],
    )
    passed = lax.ppermute(passed, "core", SWAP)
    ids_other = lax.ppermute(rel_ids, "core", SWAP)
    block = (kept + passed).reshape(plane, rows, width)
    block = exchange(block, PLANE)
    piece = jnp.sum(block.astype(F32), axis=0).astype(BF)
    pieces = exchange(copies(piece, line), LINE).reshape(line // 2, 2, rows, width)
    piece = jnp.sum(pieces.astype(F32), axis=0).astype(BF).reshape(2 * rows, width)
    own = exchange(copies(piece, plane), PLANE).reshape(n, width)
    other = lax.ppermute(own, "core", SWAP)

    heads = jnp.take(entity_table, head_ids, axis=0, mode="clip")
    angles = jnp.take(rel_phases, rel_ids, axis=0, mode="clip")
    query, cosine, sine, spot, pick = call(
        prep_kernel,
        (heads, angles, *(v.reshape(1, queries) for v in (target_pos, rel_ids, ids_other))),
        [VMEM] * 5,
        [((queries, width), BF), ((queries, half), F32), ((queries, half), F32),
         ((queries, LANES), jnp.int32), ((rel_rows, 2 * queries), BF)],
        12 * MIB, 100_000_000, 4_000_000,
    )

    loss, head_grad, keep, send, ang_keep, ang_send = call(
        main_kernel, (heads, query, own, other, spot, cosine, sine), [VMEM] * 7,
        [((1, queries), F32), ((queries, width), BF), ((n, width), F32), ((n, width), BF),
         ((queries, half // 2), F32), ((queries, half // 2), F32)],
        24 * MIB, 12 * queries * n * width, 6_000_000,
    )

    got = lax.ppermute(send, "core", SWAP)
    ang_got = lax.ppermute(ang_send, "core", SWAP)
    packed = call(
        pack_kernel, (pick, keep, got, ang_keep, ang_got), [VMEM] * 5,
        [((plane, piece_rows, LANES), BF)], 12 * MIB, 4 * rel_rows * queries * half, 4_000_000,
    )
    part = jnp.sum(exchange(packed, PLANE).astype(F32), axis=0).astype(BF)
    part = jnp.sum(exchange(copies(part, line), LINE).astype(F32), axis=0).astype(BF)
    own_sum = exchange(copies(part, plane), PLANE)
    other_sum = lax.ppermute(own_sum, "core", SWAP)
    table_grad, rel_grad = call(
        place_kernel, (block_owner, block_local, own_sum, other_sum), [SMEM, SMEM, VMEM, VMEM],
        [(entity_table.shape, BF), ((rels, half), F32)], 12 * MIB, 1_000_000, 5_000_000,
    )
    return loss.reshape(queries), head_grad, table_grad, rel_grad


def solution(mesh):
    finer = Mesh(mesh.devices.reshape(4, 4, 4, 2, mesh.shape["grp"]), ENT_GRP)
    placed = (P(ENT, None), P(), P(ENT_GRP), P(ENT_GRP), P(ENT_GRP), P(), P())
    return jax.shard_map(
        body,
        mesh=finer,
        in_specs=placed,
        out_specs=(P(ENT_GRP), P(ENT_GRP, None), P(ENT, None), P()),
        check_vma=False,
    )
```

```python
import jax
import jax.numpy as jnp
from jax import lax
from jax.experimental import pallas as pl
from jax.experimental.pallas import tpu as pltpu
from jax.sharding import Mesh
from jax.sharding import PartitionSpec as P


BLK = 128
LANES = 128
ENT = ("x", "y", "zl", "core")
ENT_GRP = ("x", "y", "zl", "core", "grp")
PLANE = ("x", "y")
LINE = ("grp", "zl")
SWAP = [(0, 1), (1, 0)]
BF = jnp.bfloat16
F32 = jnp.float32
NT = (((1,), (1,)), ((), ()))
TN = (((0,), (0,)), ((), ()))
VMEM = pl.BlockSpec(memory_space=pltpu.VMEM)
SMEM = pl.BlockSpec(memory_space=pltpu.SMEM)
HBM = pl.BlockSpec(memory_space=pltpu.HBM)
MIB = 1024 * 1024
FETCH = 56_000_000


def dot(a, b, dims=(((1,), (0,)), ((), ()))):
    return lax.dot_general(a, b, dims, preferred_element_type=F32)


def halves(x):
    hi = x.astype(BF)
    return hi, (x - hi.astype(F32)).astype(BF)


def own_shard():
    place = lax.axis_index(ENT[0])
    for axis in ENT[1:]:
        place = place * lax.axis_size(axis) + lax.axis_index(axis)
    return place


def fetch_kernel(owner_ref, local_ref, table_ref, keep_ref, pass_ref, sem):
    core = lax.axis_index("core")
    grp = lax.axis_index("grp")
    me = own_shard()
    for b, out_ref in ((2 * grp + core, keep_ref), (2 * grp + 1 - core, pass_ref)):

        @pl.when(owner_ref[b] == me)
        def _():
            start = pl.multiple_of(local_ref[b] * BLK, BLK)
            copy = pltpu.make_async_copy(table_ref.at[pl.ds(start, BLK)], out_ref, sem)
            copy.start()
            copy.wait()

        @pl.when(owner_ref[b] != me)
        def _():
            out_ref[...] = jnp.zeros_like(out_ref)


def turn_kernel(ids_ref, phases_ref, cos_ref, sin_ref):
    def take(i, carry):
        cos_ref[pl.ds(i, 1), :] = phases_ref[pl.ds(ids_ref[i], 1), :]
        return carry

    lax.fori_loop(0, cos_ref.shape[0], take, 0, unroll=8)
    angles = cos_ref[...]
    cos_ref[...] = jnp.cos(angles)
    sin_ref[...] = jnp.sin(angles)


def rotated(heads_ref, cosine, sine):
    half = cosine.shape[1]
    hr = heads_ref[:, :half].astype(F32)
    hi = heads_ref[:, half:].astype(F32)
    return hr * cosine - hi * sine, hr * sine + hi * cosine


def scored(query, cand):
    wide = cand.astype(F32)
    hi, lo = halves(wide * wide)
    ones = jnp.ones((8, cand.shape[1]), BF)
    norm = (dot(ones, hi, NT) + dot(ones, lo, NT))[:1]
    return dot(query, cand, NT) - 0.5 * norm


def early_kernel(
    heads_ref, cos_ref, sin_ref, target_ref, ids_ref, ids_other_ref, own_ref,
    query_ref, spot_ref, pick_ref, scores_ref,
):
    rows, half = cos_ref.shape
    qr, qi = rotated(heads_ref, cos_ref[...], sin_ref[...])
    query_ref[:, :half] = qr.astype(BF)
    query_ref[:, half:] = qi.astype(BF)
    scores_ref[...] = scored(query_ref[...], own_ref[...])
    t = target_ref[...]
    core = lax.axis_index("core")
    block, row = t >> 7, t & 127
    spot = (((block & 1) ^ core) << 8) + ((row >> 3) << 4) + ((block >> 1) << 3) + (row & 7)
    spot_ref[...] = jnp.broadcast_to(spot, (LANES, rows)).T
    rel = lax.broadcasted_iota(jnp.int32, (pick_ref.shape[0], rows), 0)
    pick_ref[:, :rows] = (rel == ids_ref[...]).astype(F32).astype(BF)
    pick_ref[:, rows:] = (rel == ids_other_ref[...]).astype(F32).astype(BF)


def main_kernel(
    heads_ref, query_ref, scores_ref, own_ref, other_ref, spot_ref, cos_ref, sin_ref,
    loss_ref, head_ref, keep_ref, send_ref, ang_keep_ref, ang_send_ref,
):
    rows, half = cos_ref.shape
    n = own_ref.shape[0]
    query = query_ref[...]
    cands = (own_ref[...], other_ref[...])
    spot = spot_ref[:, :1]
    scores = [scores_ref[...], scored(query, cands[1])]
    top = jnp.maximum(
        jnp.max(scores[0], axis=1, keepdims=True), jnp.max(scores[1], axis=1, keepdims=True)
    )
    exps = [jnp.exp(s - top) for s in scores]
    total = jnp.sum(exps[0], axis=1, keepdims=True) + jnp.sum(exps[1], axis=1, keepdims=True)
    lanes = lax.broadcasted_iota(jnp.int32, (rows, n), 1)
    hits = [lanes == spot, lanes + n == spot]
    picked = sum(jnp.sum(jnp.where(h, s, 0.0), axis=1, keepdims=True) for h, s in zip(hits, scores))
    loss = top + jnp.log(total) - picked
    loss_ref[...] = jnp.broadcast_to(loss, (rows, LANES)).T[:1]
    scale = 1.0 / total
    ones_q = jnp.ones((rows, LANES), BF)
    dquery = None
    for k in (1, 0):
        weights = exps[k] * scale - hits[k].astype(F32)
        low, rest = halves(weights)
        part = dot(low, cands[k])
        dquery = part if dquery is None else dquery + part
        column = (dot(low, ones_q, TN) + dot(rest, ones_q, TN))[:, :1]
        grad = dot(low, query, TN) - column * cands[k].astype(F32)
        if k == 0:
            keep_ref[...] = grad
        else:
            send_ref[...] = grad.astype(BF)
    cosine = cos_ref[...]
    sine = sin_ref[...]
    qr, qi = rotated(heads_ref, cosine, sine)
    dr, di = dquery[:, :half], dquery[:, half:]
    head_ref[:, :half] = (dr * cosine + di * sine).astype(BF)
    head_ref[:, half:] = (di * cosine - dr * sine).astype(BF)
    ang = di * qr - dr * qi
    a, b = ang[:, : half // 2], ang[:, half // 2 :]
    first = lax.axis_index("core") == 0
    ang_keep_ref[...] = jnp.where(first, a, b)
    ang_send_ref[...] = jnp.where(first, b, a)


def pack_kernel(pick_ref, keep_ref, got_ref, ang_ref, ang_got_ref, out_ref):
    pieces = out_ref.shape[0]
    per = keep_ref.shape[0] // pieces
    groups = keep_ref.shape[1] // LANES
    for k in range(groups):
        cols = slice(k * LANES, (k + 1) * LANES)
        grad = keep_ref[:, cols] + got_ref[:, cols].astype(F32)
        out_ref[:, k * per : (k + 1) * per, :] = grad.astype(BF).reshape(pieces, per, LANES)
    q = ang_ref.shape[0]
    total = None
    for k, ref in enumerate((ang_ref, ang_got_ref)):
        sel = pick_ref[:, k * q : (k + 1) * q]
        hi, lo = halves(ref[...])
        part = dot(sel, hi) + dot(sel, lo)
        total = part if total is None else total + part
    total = total.astype(BF)
    base = groups * per
    size = out_ref.shape[1] - base
    row_groups = total.shape[0] // size
    for j in range(pieces):
        at = (j % row_groups) * size
        col = (j // row_groups) * LANES
        out_ref[j, base:, :] = total[at : at + size, col : col + LANES]


def block_of(src_ref, g, k):
    per = BLK // src_ref.shape[0]
    at = (k * 2 + g) * per
    return src_ref[:, at : at + per, :].astype(F32).reshape(BLK, LANES)


def spread(src_ref, part_ref):
    pieces, piece_rows, _ = src_ref.shape
    row_groups = pieces * LANES // part_ref.shape[1]
    base = 2 * BLK * 8 // pieces
    size = piece_rows - base
    for j in range(pieces):
        at = (j % row_groups) * size
        rows = min(size, part_ref.shape[0] - at)
        col = (j // row_groups) * LANES
        part_ref[at : at + rows, col : col + LANES] = src_ref[j, base : base + rows, :].astype(F32)


def half_columns(rel_ref, part_ref, half):
    w = part_ref.shape[1]
    return rel_ref.at[:, pl.ds(pl.multiple_of(half * w, w), w)]


def place_own_kernel(owner_ref, local_ref, own_ref, table_ref, rel_ref, rows_ref, part_ref, sems):
    core = lax.axis_index("core")
    me = own_shard()
    rows_ref[...] = jnp.zeros_like(rows_ref)
    for g in range(2):
        b = 2 * g + core

        @pl.when(owner_ref[b] == me)
        def _():
            at = pl.ds(pl.multiple_of(local_ref[b] * BLK, BLK), BLK)
            for k in range(rows_ref.shape[1] // LANES):
                cols = slice(k * LANES, (k + 1) * LANES)
                old = rows_ref[at, cols].astype(F32)
                rows_ref[at, cols] = (old + block_of(own_ref, g, k)).astype(BF)

    table = pltpu.make_async_copy(rows_ref, table_ref, sems.at[0])
    table.start()
    spread(own_ref, part_ref)
    part = pltpu.make_async_copy(part_ref, half_columns(rel_ref, part_ref, core), sems.at[1])
    part.start()
    table.wait()
    part.wait()


def place_other_kernel(
    owner_ref, local_ref, own_ref, other_ref, table_in_ref, rel_in_ref,
    table_ref, rel_ref, rows_ref, sum_ref, part_ref, sems,
):
    del table_in_ref, rel_in_ref
    core = lax.axis_index("core")
    me = own_shard()
    spread(other_ref, part_ref)
    part = pltpu.make_async_copy(part_ref, half_columns(rel_ref, part_ref, 1 - core), sems.at[2])
    part.start()
    groups = rows_ref.shape[2] // LANES
    for g in range(2):
        b = 2 * g + 1 - core

        @pl.when(owner_ref[b] == me)
        def _():
            for k in range(groups):
                cols = slice(k * LANES, (k + 1) * LANES)
                sum_ref[:, cols] = block_of(other_ref, g, k)
            twins = ((own_ref, core, 0), (own_ref, 2 + core, 1), (other_ref, 2 * (1 - g) + 1 - core, 1 - g))
            for src_ref, c, h in twins:

                @pl.when((owner_ref[c] == me) & (local_ref[c] == local_ref[b]))
                def _():
                    for k in range(groups):
                        cols = slice(k * LANES, (k + 1) * LANES)
                        sum_ref[:, cols] = sum_ref[:, cols] + block_of(src_ref, h, k)

            rows_ref[g] = sum_ref[...].astype(BF)
            at = pl.ds(pl.multiple_of(local_ref[b] * BLK, BLK), BLK)
            copy = pltpu.make_async_copy(rows_ref.at[g], table_ref.at[at], sems.at[g])
            copy.start()
            copy.wait()

    part.wait()


def exchange(x, axes):
    return lax.all_to_all(x, axes, split_axis=0, concat_axis=0, tiled=True)


def copies(x, n):
    return jnp.broadcast_to(x[None], (n, *x.shape))


def call(kernel, ins, specs, outs, grant, flops, nbytes, scratch=(), out=VMEM, aliases=None):
    shapes = tuple(jax.ShapeDtypeStruct(s, d) for s, d in outs)
    single = len(shapes) == 1
    return pl.pallas_call(
        kernel,
        out_shape=shapes[0] if single else shapes,
        in_specs=specs,
        out_specs=out if single else (out,) * len(shapes),
        scratch_shapes=list(scratch),
        input_output_aliases=aliases or {},
        compiler_params=pltpu.CompilerParams(vmem_limit_bytes=grant),
        cost_estimate=pl.CostEstimate(flops=flops, bytes_accessed=nbytes, transcendentals=0),
    )(*ins)


def body(entity_table, rel_phases, head_ids, rel_ids, target_pos, block_owner, block_local):
    half = rel_phases.shape[1]
    rels = rel_phases.shape[0]
    width = 2 * half
    queries = head_ids.shape[0]
    plane = lax.axis_size(PLANE)
    line = lax.axis_size(LINE)
    rows = BLK // plane
    n = 2 * BLK
    rel_rows = -(-rels // 64) * 64
    piece_rows = n * width // (plane * LANES) + rel_rows * half // 2 // (plane * LANES)

    kept, passed = call(
        fetch_kernel, (block_owner, block_local, entity_table), [SMEM, SMEM, HBM],
        [((BLK, width), BF)] * 2, FETCH, 100_000, 500_000, [pltpu.SemaphoreType.DMA],
    )
    passed = lax.ppermute(passed, "core", SWAP)
    ids_other = lax.ppermute(rel_ids, "core", SWAP)
    block = (kept + passed).reshape(plane, rows, width)
    block = exchange(block, PLANE)
    piece = jnp.sum(block.astype(F32), axis=0).astype(BF)
    pieces = exchange(copies(piece, line), LINE).reshape(2, line // 2, rows, width)
    piece = jnp.sum(pieces.astype(F32), axis=1).astype(BF).reshape(2 * rows, width)
    own = exchange(copies(piece, plane), PLANE).reshape(n, width)
    other = lax.ppermute(own, "core", SWAP)

    heads = jnp.take(entity_table, head_ids, axis=0, mode="clip")
    cosine, sine = call(
        turn_kernel, (rel_ids, rel_phases), [SMEM, VMEM], [((queries, half), F32)] * 2,
        8 * MIB, 10_000_000, 2_000_000,
    )
    query, spot, pick, scores = call(
        early_kernel,
        (heads, cosine, sine, *(v.reshape(1, queries) for v in (target_pos, rel_ids, ids_other)), own),
        [VMEM] * 7,
        [((queries, width), BF), ((queries, LANES), jnp.int32), ((rel_rows, 2 * queries), BF),
         ((queries, n), F32)],
        12 * MIB, 4 * queries * n * width, 4_000_000,
    )

    loss, head_grad, keep, send, ang_keep, ang_send = call(
        main_kernel, (heads, query, scores, own, other, spot, cosine, sine), [VMEM] * 8,
        [((1, queries), F32), ((queries, width), BF), ((n, width), F32), ((n, width), BF),
         ((queries, half // 2), F32), ((queries, half // 2), F32)],
        24 * MIB, 10 * queries * n * width, 6_000_000,
    )

    got = lax.ppermute(send, "core", SWAP)
    ang_got = lax.ppermute(ang_send, "core", SWAP)
    packed = call(
        pack_kernel, (pick, keep, got, ang_keep, ang_got), [VMEM] * 5,
        [((plane, piece_rows, LANES), BF)], 12 * MIB, 4 * rel_rows * queries * half, 4_000_000,
    )
    part = jnp.sum(exchange(packed, PLANE).astype(F32), axis=0).astype(BF)
    part = jnp.sum(exchange(copies(part, line), LINE).astype(F32), axis=0).astype(BF)
    own_sum = exchange(copies(part, plane), PLANE)
    other_sum = lax.ppermute(own_sum, "core", SWAP)
    shapes = [(entity_table.shape, BF), ((rels, half), F32)]
    part = pltpu.VMEM((rels, half // 2), F32)
    partial = call(
        place_own_kernel, (block_owner, block_local, own_sum), [SMEM, SMEM, VMEM], shapes,
        8 * MIB, 1_000_000, 2_000_000,
        [pltpu.VMEM(entity_table.shape, BF), part, pltpu.SemaphoreType.DMA((2,))], HBM,
    )
    table_grad, rel_grad = call(
        place_other_kernel, (block_owner, block_local, own_sum, other_sum, *partial),
        [SMEM, SMEM, VMEM, VMEM, HBM, HBM], shapes, 8 * MIB, 1_000_000, 2_000_000,
        [pltpu.VMEM((2, BLK, width), BF), pltpu.VMEM((BLK, width), F32), part,
         pltpu.SemaphoreType.DMA((3,))],
        HBM, {4: 0, 5: 1},
    )
    return loss.reshape(queries), head_grad, table_grad, rel_grad


def solution(mesh):
    finer = Mesh(mesh.devices.reshape(4, 4, 4, 2, mesh.shape["grp"]), ENT_GRP)
    placed = (P(ENT, None), P(), P(ENT_GRP), P(ENT_GRP), P(ENT_GRP), P(), P())
    return jax.shard_map(
        body,
        mesh=finer,
        in_specs=placed,
        out_specs=(P(ENT_GRP), P(ENT_GRP, None), P(ENT, None), P()),
        check_vma=False,
    )
```

```python
import jax
import jax.numpy as jnp
from jax import lax
from jax.experimental import pallas as pl
from jax.experimental.pallas import tpu as pltpu
from jax.sharding import Mesh
from jax.sharding import PartitionSpec as P


BLK = 128
LANES = 128
ENT = ("x", "y", "zl", "core")
ENT_GRP = ("x", "y", "zl", "core", "grp")
PLANE = ("x", "y")
LINE = ("grp", "zl")
SWAP = [(0, 1), (1, 0)]
BF = jnp.bfloat16
F32 = jnp.float32
NT = (((1,), (1,)), ((), ()))
TN = (((0,), (0,)), ((), ()))
VMEM = pl.BlockSpec(memory_space=pltpu.VMEM)
SMEM = pl.BlockSpec(memory_space=pltpu.SMEM)
HBM = pl.BlockSpec(memory_space=pltpu.HBM)
MIB = 1024 * 1024
FETCH = 56_000_000


def dot(a, b, dims=(((1,), (0,)), ((), ()))):
    return lax.dot_general(a, b, dims, preferred_element_type=F32)


def halves(x):
    hi = x.astype(BF)
    return hi, (x - hi.astype(F32)).astype(BF)


def own_shard():
    place = lax.axis_index(ENT[0])
    for axis in ENT[1:]:
        place = place * lax.axis_size(axis) + lax.axis_index(axis)
    return place


def fetch_kernel(number_ref, table_ref, keep_ref, pass_ref, sem):
    core = lax.axis_index("core")
    grp = lax.axis_index("grp")
    me = own_shard()
    per = table_ref.shape[0] // BLK
    for b, out_ref in ((2 * grp + core, keep_ref), (2 * grp + 1 - core, pass_ref)):

        @pl.when(number_ref[b] // per == me)
        def _():
            start = pl.multiple_of(number_ref[b] % per * BLK, BLK)
            copy = pltpu.make_async_copy(table_ref.at[pl.ds(start, BLK)], out_ref, sem)
            copy.start()
            copy.wait()

        @pl.when(number_ref[b] // per != me)
        def _():
            out_ref[...] = jnp.zeros_like(out_ref)


def cos_sin(x):
    turns = jnp.floor(x * 0.6366197723675814 + 0.5)
    rest = ((x - turns * 1.5703125) - turns * 4.837512969970703125e-4) - turns * 7.54978995489188e-8
    z = rest * rest
    s = ((-1.9515295891e-4 * z + 8.3321608736e-3) * z - 1.6666654611e-1) * z * rest + rest
    c = ((2.443315711809948e-5 * z - 1.388731625493765e-3) * z + 4.166664568298827e-2) * z * z
    c = c - 0.5 * z + 1.0
    quarter = turns.astype(jnp.int32)
    odd = (quarter & 1) != 0
    cosine = jnp.where(odd, s, c)
    sine = jnp.where(odd, c, s)
    cosine = jnp.where(((quarter + 1) & 2) != 0, -cosine, cosine)
    sine = jnp.where((quarter & 2) != 0, -sine, sine)
    return cosine, sine


def turn_kernel(ids_ref, phases_ref, cos_ref, sin_ref):
    def take(i, carry):
        cos_ref[pl.ds(i, 1), :] = phases_ref[pl.ds(ids_ref[i], 1), :]
        return carry

    lax.fori_loop(0, cos_ref.shape[0], take, 0, unroll=16)
    cosine, sine = cos_sin(cos_ref[...])
    cos_ref[...] = cosine
    sin_ref[...] = sine


def rotated(heads_ref, cosine, sine):
    half = cosine.shape[1]
    hr = heads_ref[:, :half].astype(F32)
    hi = heads_ref[:, half:].astype(F32)
    return hr * cosine - hi * sine, hr * sine + hi * cosine


def scored(query, cand):
    wide = cand.astype(F32)
    hi, lo = halves(wide * wide)
    ones = jnp.ones((8, cand.shape[1]), BF)
    norm = (dot(ones, hi, NT) + dot(ones, lo, NT))[:1]
    return dot(query, cand, NT) - 0.5 * norm


def early_kernel(
    heads_ref, cos_ref, sin_ref, target_ref, ids_ref, ids_other_ref, own_ref,
    query_ref, spot_ref, pick_ref, scores_ref,
):
    rows, half = cos_ref.shape
    qr, qi = rotated(heads_ref, cos_ref[...], sin_ref[...])
    query_ref[:, :half] = qr.astype(BF)
    query_ref[:, half:] = qi.astype(BF)
    scores_ref[...] = scored(query_ref[...], own_ref[...])
    t = target_ref[...]
    core = lax.axis_index("core")
    block, row = t >> 7, t & 127
    spot = (((block & 1) ^ core) << 8) + ((row >> 3) << 4) + ((block >> 1) << 3) + (row & 7)
    spot_ref[...] = jnp.broadcast_to(spot, (LANES, rows)).T
    rel = lax.broadcasted_iota(jnp.int32, (pick_ref.shape[0], rows), 0)
    pick_ref[:, :rows] = (rel == ids_ref[...]).astype(F32).astype(BF)
    pick_ref[:, rows:] = (rel == ids_other_ref[...]).astype(F32).astype(BF)


def main_kernel(
    heads_ref, query_ref, scores_ref, own_ref, other_ref, spot_ref, cos_ref, sin_ref,
    loss_ref, head_ref, keep_ref, send_ref, ang_keep_ref, ang_send_ref,
):
    rows, half = cos_ref.shape
    n = own_ref.shape[0]
    query = query_ref[...]
    cands = (own_ref[...], other_ref[...])
    spot = spot_ref[:, :1]
    scores = [scores_ref[...], scored(query, cands[1])]
    top = jnp.maximum(
        jnp.max(scores[0], axis=1, keepdims=True), jnp.max(scores[1], axis=1, keepdims=True)
    )
    exps = [jnp.exp(s - top) for s in scores]
    total = jnp.sum(exps[0], axis=1, keepdims=True) + jnp.sum(exps[1], axis=1, keepdims=True)
    lanes = lax.broadcasted_iota(jnp.int32, (rows, n), 1)
    hits = [lanes == spot, lanes + n == spot]
    picked = sum(jnp.sum(jnp.where(h, s, 0.0), axis=1, keepdims=True) for h, s in zip(hits, scores))
    loss = top + jnp.log(total) - picked
    loss_ref[...] = jnp.broadcast_to(loss, (rows, LANES)).T[:1]
    scale = 1.0 / total
    ones_q = jnp.ones((rows, LANES), BF)
    dquery = None
    for k in (1, 0):
        weights = exps[k] * scale - hits[k].astype(F32)
        low, rest = halves(weights)
        part = dot(low, cands[k])
        dquery = part if dquery is None else dquery + part
        column = (dot(low, ones_q, TN) + dot(rest, ones_q, TN))[:, :1]
        grad = dot(low, query, TN) - column * cands[k].astype(F32)
        if k == 0:
            keep_ref[...] = grad
        else:
            send_ref[...] = grad.astype(BF)
    cosine = cos_ref[...]
    sine = sin_ref[...]
    qr, qi = rotated(heads_ref, cosine, sine)
    dr, di = dquery[:, :half], dquery[:, half:]
    head_ref[:, :half] = (dr * cosine + di * sine).astype(BF)
    head_ref[:, half:] = (di * cosine - dr * sine).astype(BF)
    ang = di * qr - dr * qi
    a, b = ang[:, : half // 2], ang[:, half // 2 :]
    first = lax.axis_index("core") == 0
    ang_keep_ref[...] = jnp.where(first, a, b)
    ang_send_ref[...] = jnp.where(first, b, a)


def pack_kernel(pick_ref, keep_ref, got_ref, ang_ref, ang_got_ref, out_ref):
    pieces = out_ref.shape[0]
    per = keep_ref.shape[0] // pieces
    groups = keep_ref.shape[1] // LANES
    for k in range(groups):
        cols = slice(k * LANES, (k + 1) * LANES)
        grad = keep_ref[:, cols] + got_ref[:, cols].astype(F32)
        out_ref[:, k * per : (k + 1) * per, :] = grad.astype(BF).reshape(pieces, per, LANES)
    q = ang_ref.shape[0]
    total = None
    for k, ref in enumerate((ang_ref, ang_got_ref)):
        sel = pick_ref[:, k * q : (k + 1) * q]
        hi, lo = halves(ref[...])
        part = dot(sel, hi) + dot(sel, lo)
        total = part if total is None else total + part
    total = total.astype(BF)
    base = groups * per
    size = out_ref.shape[1] - base
    row_groups = total.shape[0] // size
    for j in range(pieces):
        at = (j % row_groups) * size
        col = (j // row_groups) * LANES
        out_ref[j, base:, :] = total[at : at + size, col : col + LANES]


def block_of(src_ref, g, k):
    per = BLK // src_ref.shape[0]
    at = (k * 2 + g) * per
    return src_ref[:, at : at + per, :].astype(F32).reshape(BLK, LANES)


def spread(src_ref, part_ref):
    pieces, piece_rows, _ = src_ref.shape
    row_groups = pieces * LANES // part_ref.shape[1]
    base = 2 * BLK * 8 // pieces
    size = piece_rows - base
    for j in range(pieces):
        at = (j % row_groups) * size
        rows = min(size, part_ref.shape[0] - at)
        col = (j // row_groups) * LANES
        part_ref[at : at + rows, col : col + LANES] = src_ref[j, base : base + rows, :].astype(F32)


def half_columns(rel_ref, part_ref, half):
    w = part_ref.shape[1]
    return rel_ref.at[:, pl.ds(pl.multiple_of(half * w, w), w)]


def place_own_kernel(number_ref, own_ref, table_ref, rel_ref, rows_ref, part_ref, sems):
    core = lax.axis_index("core")
    me = own_shard()
    per = table_ref.shape[0] // BLK
    rows_ref[...] = jnp.zeros_like(rows_ref)
    for g in range(2):
        b = 2 * g + core

        @pl.when(number_ref[b] // per == me)
        def _():
            at = pl.ds(pl.multiple_of(number_ref[b] % per * BLK, BLK), BLK)
            for k in range(rows_ref.shape[1] // LANES):
                cols = slice(k * LANES, (k + 1) * LANES)
                old = rows_ref[at, cols].astype(F32)
                rows_ref[at, cols] = (old + block_of(own_ref, g, k)).astype(BF)

    table = pltpu.make_async_copy(rows_ref, table_ref, sems.at[0])
    table.start()
    spread(own_ref, part_ref)
    part = pltpu.make_async_copy(part_ref, half_columns(rel_ref, part_ref, core), sems.at[1])
    part.start()
    table.wait()
    part.wait()


def place_other_kernel(
    number_ref, own_ref, other_ref, table_in_ref, rel_in_ref,
    table_ref, rel_ref, rows_ref, sum_ref, part_ref, sems,
):
    del table_in_ref, rel_in_ref
    core = lax.axis_index("core")
    me = own_shard()
    spread(other_ref, part_ref)
    part = pltpu.make_async_copy(part_ref, half_columns(rel_ref, part_ref, 1 - core), sems.at[2])
    part.start()
    per = table_ref.shape[0] // BLK
    groups = rows_ref.shape[2] // LANES
    for g in range(2):
        b = 2 * g + 1 - core

        @pl.when(number_ref[b] // per == me)
        def _():
            for k in range(groups):
                cols = slice(k * LANES, (k + 1) * LANES)
                sum_ref[:, cols] = block_of(other_ref, g, k)
            twins = ((own_ref, core, 0), (own_ref, 2 + core, 1), (other_ref, 2 * (1 - g) + 1 - core, 1 - g))
            for src_ref, c, h in twins:

                @pl.when(number_ref[c] == number_ref[b])
                def _():
                    for k in range(groups):
                        cols = slice(k * LANES, (k + 1) * LANES)
                        sum_ref[:, cols] = sum_ref[:, cols] + block_of(src_ref, h, k)

            rows_ref[g] = sum_ref[...].astype(BF)
            at = pl.ds(pl.multiple_of(number_ref[b] % per * BLK, BLK), BLK)
            copy = pltpu.make_async_copy(rows_ref.at[g], table_ref.at[at], sems.at[g])
            copy.start()
            copy.wait()

    part.wait()


def exchange(x, axes):
    return lax.all_to_all(x, axes, split_axis=0, concat_axis=0, tiled=True)


def copies(x, n):
    return jnp.broadcast_to(x[None], (n, *x.shape))


def call(kernel, ins, specs, outs, grant, flops, nbytes, scratch=(), out=VMEM, aliases=None):
    shapes = tuple(jax.ShapeDtypeStruct(s, d) for s, d in outs)
    single = len(shapes) == 1
    return pl.pallas_call(
        kernel,
        out_shape=shapes[0] if single else shapes,
        in_specs=specs,
        out_specs=out if single else (out,) * len(shapes),
        scratch_shapes=list(scratch),
        input_output_aliases=aliases or {},
        compiler_params=pltpu.CompilerParams(vmem_limit_bytes=grant),
        cost_estimate=pl.CostEstimate(flops=flops, bytes_accessed=nbytes, transcendentals=0),
    )(*ins)


def body(entity_table, rel_phases, head_ids, rel_ids, target_pos, block_owner, block_local):
    half = rel_phases.shape[1]
    rels = rel_phases.shape[0]
    width = 2 * half
    queries = head_ids.shape[0]
    plane = lax.axis_size(PLANE)
    line = lax.axis_size(LINE)
    rows = BLK // plane
    n = 2 * BLK
    rel_rows = -(-rels // 64) * 64
    piece_rows = n * width // (plane * LANES) + rel_rows * half // 2 // (plane * LANES)

    numbers = block_owner * (entity_table.shape[0] // BLK) + block_local
    kept, passed = call(
        fetch_kernel, (numbers, entity_table), [SMEM, HBM],
        [((BLK, width), BF)] * 2, FETCH, 100_000, 500_000, [pltpu.SemaphoreType.DMA],
    )
    passed = lax.ppermute(passed, "core", SWAP)
    ids_other = lax.ppermute(rel_ids, "core", SWAP)
    block = (kept + passed).reshape(plane, rows, width)
    block = exchange(block, PLANE)
    piece = jnp.sum(block.astype(F32), axis=0).astype(BF)
    pieces = exchange(copies(piece, line), LINE).reshape(2, line // 2, rows, width)
    piece = jnp.sum(pieces.astype(F32), axis=1).astype(BF).reshape(2 * rows, width)
    own = exchange(copies(piece, plane), PLANE).reshape(n, width)
    other = lax.ppermute(own, "core", SWAP)

    heads = jnp.take(entity_table, head_ids, axis=0, mode="clip")
    cosine, sine = call(
        turn_kernel, (rel_ids, rel_phases), [SMEM, VMEM], [((queries, half), F32)] * 2,
        8 * MIB, 10_000_000, 2_000_000,
    )
    query, spot, pick, scores = call(
        early_kernel,
        (heads, cosine, sine, *(v.reshape(1, queries) for v in (target_pos, rel_ids, ids_other)), own),
        [VMEM] * 7,
        [((queries, width), BF), ((queries, LANES), jnp.int32), ((rel_rows, 2 * queries), BF),
         ((queries, n), F32)],
        12 * MIB, 4 * queries * n * width, 4_000_000,
    )

    loss, head_grad, keep, send, ang_keep, ang_send = call(
        main_kernel, (heads, query, scores, own, other, spot, cosine, sine), [VMEM] * 8,
        [((1, queries), F32), ((queries, width), BF), ((n, width), F32), ((n, width), BF),
         ((queries, half // 2), F32), ((queries, half // 2), F32)],
        24 * MIB, 10 * queries * n * width, 6_000_000,
    )

    got = lax.ppermute(send, "core", SWAP)
    ang_got = lax.ppermute(ang_send, "core", SWAP)
    packed = call(
        pack_kernel, (pick, keep, got, ang_keep, ang_got), [VMEM] * 5,
        [((plane, piece_rows, LANES), BF)], 12 * MIB, 4 * rel_rows * queries * half, 4_000_000,
    )
    part = jnp.sum(exchange(packed, PLANE).astype(F32), axis=0).astype(BF)
    part = jnp.sum(exchange(copies(part, line), LINE).astype(F32), axis=0).astype(BF)
    own_sum = exchange(copies(part, plane), PLANE)
    other_sum = lax.ppermute(own_sum, "core", SWAP)
    shapes = [(entity_table.shape, BF), ((rels, half), F32)]
    part = pltpu.VMEM((rels, half // 2), F32)
    partial = call(
        place_own_kernel, (numbers, own_sum), [SMEM, VMEM], shapes,
        8 * MIB, 1_000_000, 2_000_000,
        [pltpu.VMEM(entity_table.shape, BF), part, pltpu.SemaphoreType.DMA((2,))], HBM,
    )
    table_grad, rel_grad = call(
        place_other_kernel, (numbers, own_sum, other_sum, *partial),
        [SMEM, VMEM, VMEM, HBM, HBM], shapes, 8 * MIB, 1_000_000, 2_000_000,
        [pltpu.VMEM((2, BLK, width), BF), pltpu.VMEM((BLK, width), F32), part,
         pltpu.SemaphoreType.DMA((3,))],
        HBM, {3: 0, 4: 1},
    )
    return loss.reshape(queries), head_grad, table_grad, rel_grad


def solution(mesh):
    finer = Mesh(mesh.devices.reshape(4, 4, 4, 2, mesh.shape["grp"]), ENT_GRP)
    placed = (P(ENT, None), P(), P(ENT_GRP), P(ENT_GRP), P(ENT_GRP), P(), P())
    return jax.shard_map(
        body,
        mesh=finer,
        in_specs=placed,
        out_specs=(P(ENT_GRP), P(ENT_GRP, None), P(ENT, None), P()),
        check_vma=False,
    )
```

```python
import jax
import jax.numpy as jnp
from jax import lax
from jax.experimental import pallas as pl
from jax.experimental.pallas import tpu as pltpu
from jax.sharding import Mesh
from jax.sharding import PartitionSpec as P


BLK = 128
LANES = 128
ENT = ("x", "y", "zl", "core")
ENT_GRP = ("x", "y", "zl", "core", "grp")
PLANE = ("x", "y")
LINE = ("grp", "zl")
SWAP = [(0, 1), (1, 0)]
BF = jnp.bfloat16
F32 = jnp.float32
NT = (((1,), (1,)), ((), ()))
TN = (((0,), (0,)), ((), ()))
VMEM = pl.BlockSpec(memory_space=pltpu.VMEM)
SMEM = pl.BlockSpec(memory_space=pltpu.SMEM)
ANY = pl.BlockSpec(memory_space=pl.ANY)
HBM = pl.BlockSpec(memory_space=pltpu.HBM)
MIB = 1024 * 1024
FETCH = 56_000_000


def dot(a, b, dims=(((1,), (0,)), ((), ()))):
    return lax.dot_general(a, b, dims, preferred_element_type=F32)


def halves(x):
    hi = x.astype(BF)
    return hi, (x - hi.astype(F32)).astype(BF)


def own_shard():
    place = lax.axis_index(ENT[0])
    for axis in ENT[1:]:
        place = place * lax.axis_size(axis) + lax.axis_index(axis)
    return place


def fetch_kernel(number_ref, table_ref, keep_ref, pass_ref, sem):
    core = lax.axis_index("core")
    grp = lax.axis_index("grp")
    me = own_shard()
    per = table_ref.shape[0] // BLK
    for b, out_ref in ((2 * grp + core, keep_ref), (2 * grp + 1 - core, pass_ref)):

        @pl.when(number_ref[b] // per == me)
        def _():
            start = pl.multiple_of(number_ref[b] % per * BLK, BLK)
            copy = pltpu.make_async_copy(table_ref.at[pl.ds(start, BLK)], out_ref, sem)
            copy.start()
            copy.wait()

        @pl.when(number_ref[b] // per != me)
        def _():
            out_ref[...] = jnp.zeros_like(out_ref)


def cos_sin(x):
    turns = jnp.floor(x * 0.6366197723675814 + 0.5)
    rest = ((x - turns * 1.5703125) - turns * 4.837512969970703125e-4) - turns * 7.54978995489188e-8
    z = rest * rest
    s = ((-1.9515295891e-4 * z + 8.3321608736e-3) * z - 1.6666654611e-1) * z * rest + rest
    c = ((2.443315711809948e-5 * z - 1.388731625493765e-3) * z + 4.166664568298827e-2) * z * z
    c = c - 0.5 * z + 1.0
    quarter = turns.astype(jnp.int32)
    odd = (quarter & 1) != 0
    cosine = jnp.where(odd, s, c)
    sine = jnp.where(odd, c, s)
    cosine = jnp.where(((quarter + 1) & 2) != 0, -cosine, cosine)
    sine = jnp.where((quarter & 2) != 0, -sine, sine)
    return cosine, sine


def turn_kernel(ids_ref, phases_ref, cos_ref, sin_ref):
    def take(i, carry):
        cos_ref[pl.ds(i, 1), :] = phases_ref[pl.ds(ids_ref[i], 1), :]
        return carry

    lax.fori_loop(0, cos_ref.shape[0], take, 0, unroll=16)
    cosine, sine = cos_sin(cos_ref[...])
    cos_ref[...] = cosine
    sin_ref[...] = sine


def rotated(heads_ref, cosine, sine):
    half = cosine.shape[1]
    hr = heads_ref[:, :half].astype(F32)
    hi = heads_ref[:, half:].astype(F32)
    return hr * cosine - hi * sine, hr * sine + hi * cosine


def scored(query, cand):
    wide = cand.astype(F32)
    hi, lo = halves(wide * wide)
    ones = jnp.ones((8, cand.shape[1]), BF)
    norm = (dot(ones, hi, NT) + dot(ones, lo, NT))[:1]
    return dot(query, cand, NT) - 0.5 * norm


def early_kernel(
    heads_ref, cos_ref, sin_ref, target_ref, ids_ref, ids_other_ref, own_ref,
    query_ref, spot_ref, pick_ref, scores_ref,
):
    rows, half = cos_ref.shape
    qr, qi = rotated(heads_ref, cos_ref[...], sin_ref[...])
    query_ref[:, :half] = qr.astype(BF)
    query_ref[:, half:] = qi.astype(BF)
    scores_ref[...] = scored(query_ref[...], own_ref[...])
    t = target_ref[...]
    core = lax.axis_index("core")
    block, row = t >> 7, t & 127
    spot = (((block & 1) ^ core) << 8) + ((row >> 3) << 4) + ((block >> 1) << 3) + (row & 7)
    spot_ref[...] = jnp.broadcast_to(spot, (LANES, rows)).T
    rel = lax.broadcasted_iota(jnp.int32, (pick_ref.shape[0], rows), 0)
    pick_ref[:, :rows] = (rel == ids_ref[...]).astype(F32).astype(BF)
    pick_ref[:, rows:] = (rel == ids_other_ref[...]).astype(F32).astype(BF)


def main_kernel(
    heads_ref, query_ref, scores_ref, own_ref, other_ref, spot_ref, cos_ref, sin_ref,
    loss_ref, dquery_ref, send_ref, ang_keep_ref, ang_send_ref, low_ref, rest_ref,
):
    rows, half = cos_ref.shape
    n = own_ref.shape[0]
    query = query_ref[...]
    cands = (own_ref[...], other_ref[...])
    spot = spot_ref[:, :1]
    scores = [scores_ref[...], scored(query, cands[1])]
    top = jnp.maximum(
        jnp.max(scores[0], axis=1, keepdims=True), jnp.max(scores[1], axis=1, keepdims=True)
    )
    exps = [jnp.exp(s - top) for s in scores]
    total = jnp.sum(exps[0], axis=1, keepdims=True) + jnp.sum(exps[1], axis=1, keepdims=True)
    lanes = lax.broadcasted_iota(jnp.int32, (rows, n), 1)
    hits = [lanes == spot, lanes + n == spot]
    picked = sum(jnp.sum(jnp.where(h, s, 0.0), axis=1, keepdims=True) for h, s in zip(hits, scores))
    loss = top + jnp.log(total) - picked
    loss_ref[...] = jnp.broadcast_to(loss, (rows, LANES)).T[:1]
    scale = 1.0 / total
    dquery = None
    for k in (1, 0):
        weights = exps[k] * scale - hits[k].astype(F32)
        low, rest = halves(weights)
        part = dot(low, cands[k])
        dquery = part if dquery is None else dquery + part
        if k == 0:
            low_ref[...] = low
            rest_ref[...] = rest
        else:
            send_ref[...] = pulled(low, rest, query, cands[k]).astype(BF)
    cosine = cos_ref[...]
    sine = sin_ref[...]
    qr, qi = rotated(heads_ref, cosine, sine)
    dr, di = dquery[:, :half], dquery[:, half:]
    dquery_ref[...] = dquery
    ang = di * qr - dr * qi
    a, b = ang[:, : half // 2], ang[:, half // 2 :]
    first = lax.axis_index("core") == 0
    ang_keep_ref[...] = jnp.where(first, a, b)
    ang_send_ref[...] = jnp.where(first, b, a)


def pulled(low, rest, query, cand):
    ones = jnp.ones((low.shape[0], LANES), BF)
    column = (dot(low, ones, TN) + dot(rest, ones, TN))[:, :1]
    return dot(low, query, TN) - column * cand.astype(F32)


def keep_kernel(
    loss_in_ref, dquery_ref, cos_ref, sin_ref, low_ref, rest_ref, query_ref, own_ref, pick_ref, ang_ref,
    loss_ref, head_ref, keep_ref, rel_ref,
):
    half = cos_ref.shape[1]
    loss_ref[...] = loss_in_ref[...]
    cosine = cos_ref[...]
    sine = sin_ref[...]
    dr, di = dquery_ref[:, :half], dquery_ref[:, half:]
    head_ref[:, :half] = (dr * cosine + di * sine).astype(BF)
    head_ref[:, half:] = (di * cosine - dr * sine).astype(BF)
    keep_ref[...] = pulled(low_ref[...], rest_ref[...], query_ref[...], own_ref[...])
    hi, lo = halves(ang_ref[...])
    sel = pick_ref[:, : ang_ref.shape[0]]
    rel_ref[...] = dot(sel, hi) + dot(sel, lo)


def pack_kernel(pick_ref, keep_ref, got_ref, rel_ref, ang_got_ref, out_ref):
    pieces = out_ref.shape[0]
    per = keep_ref.shape[0] // pieces
    groups = keep_ref.shape[1] // LANES
    for k in range(groups):
        cols = slice(k * LANES, (k + 1) * LANES)
        grad = keep_ref[:, cols] + got_ref[:, cols].astype(F32)
        out_ref[:, k * per : (k + 1) * per, :] = grad.astype(BF).reshape(pieces, per, LANES)
    hi, lo = halves(ang_got_ref[...])
    sel = pick_ref[:, ang_got_ref.shape[0] :]
    total = (rel_ref[...] + (dot(sel, hi) + dot(sel, lo))).astype(BF)
    base = groups * per
    size = out_ref.shape[1] - base
    row_groups = total.shape[0] // size
    for j in range(pieces):
        at = (j % row_groups) * size
        col = (j // row_groups) * LANES
        out_ref[j, base:, :] = total[at : at + size, col : col + LANES]


def block_of(src_ref, g, k):
    per = BLK // src_ref.shape[0]
    at = (k * 2 + g) * per
    return src_ref[:, at : at + per, :].astype(F32).reshape(BLK, LANES)


def spread(src_ref, part_ref):
    pieces, piece_rows, _ = src_ref.shape
    row_groups = pieces * LANES // part_ref.shape[1]
    base = 2 * BLK * 8 // pieces
    size = piece_rows - base
    for j in range(pieces):
        at = (j % row_groups) * size
        rows = min(size, part_ref.shape[0] - at)
        col = (j // row_groups) * LANES
        part_ref[at : at + rows, col : col + LANES] = src_ref[j, base : base + rows, :].astype(F32)


def half_columns(rel_ref, part_ref, half):
    w = part_ref.shape[1]
    return rel_ref.at[:, pl.ds(pl.multiple_of(half * w, w), w)]


def place_own_kernel(
    numbers_ref, own_ref, table_ref, rel_ref, rows_ref, part_ref, number_ref, sems
):
    core = lax.axis_index("core")
    me = own_shard()
    per = table_ref.shape[0] // BLK
    load = pltpu.make_async_copy(numbers_ref, number_ref, sems.at[2])
    load.start()
    spread(own_ref, part_ref)
    part = pltpu.make_async_copy(part_ref, half_columns(rel_ref, part_ref, core), sems.at[1])
    part.start()
    rows_ref[...] = jnp.zeros_like(rows_ref)
    load.wait()
    for g in range(2):
        b = 2 * g + core

        @pl.when(number_ref[b] // per == me)
        def _():
            at = pl.ds(pl.multiple_of(number_ref[b] % per * BLK, BLK), BLK)
            for k in range(rows_ref.shape[1] // LANES):
                cols = slice(k * LANES, (k + 1) * LANES)
                old = rows_ref[at, cols].astype(F32)
                rows_ref[at, cols] = (old + block_of(own_ref, g, k)).astype(BF)

    table = pltpu.make_async_copy(rows_ref, table_ref, sems.at[0])
    table.start()
    table.wait()
    part.wait()


def place_other_kernel(
    numbers_ref, own_ref, other_ref, table_in_ref, rel_in_ref,
    table_ref, rel_ref, rows_ref, sum_ref, part_ref, number_ref, sems,
):
    del table_in_ref, rel_in_ref
    core = lax.axis_index("core")
    me = own_shard()
    per = table_ref.shape[0] // BLK
    groups = rows_ref.shape[2] // LANES
    load = pltpu.make_async_copy(numbers_ref, number_ref, sems.at[3])
    load.start()
    spread(other_ref, part_ref)
    part = pltpu.make_async_copy(part_ref, half_columns(rel_ref, part_ref, 1 - core), sems.at[2])
    part.start()
    load.wait()
    blocks = []
    for g in range(2):
        b = 2 * g + 1 - core
        at = pl.ds(pl.multiple_of(number_ref[b] % per * BLK, BLK), BLK)
        copy = pltpu.make_async_copy(rows_ref.at[g], table_ref.at[at], sems.at[g])
        mine = number_ref[b] // per == me
        if g == 1:
            mine = mine & (number_ref[b] != number_ref[1 - core])
        blocks.append((mine, copy))

        @pl.when(mine)
        def _():
            for k in range(groups):
                cols = slice(k * LANES, (k + 1) * LANES)
                sum_ref[:, cols] = block_of(other_ref, g, k)
            twins = ((own_ref, core, 0), (own_ref, 2 + core, 1), (other_ref, 2 * (1 - g) + 1 - core, 1 - g))
            for src_ref, c, h in twins:

                @pl.when(number_ref[c] == number_ref[b])
                def _():
                    for k in range(groups):
                        cols = slice(k * LANES, (k + 1) * LANES)
                        sum_ref[:, cols] = sum_ref[:, cols] + block_of(src_ref, h, k)

            rows_ref[g] = sum_ref[...].astype(BF)
            copy.start()

    for mine, copy in blocks:
        pl.when(mine)(copy.wait)
    part.wait()


def exchange(x, axes):
    return lax.all_to_all(x, axes, split_axis=0, concat_axis=0, tiled=True)


def copies(x, n):
    return jnp.broadcast_to(x[None], (n, *x.shape))


def call(kernel, ins, specs, outs, grant, flops, nbytes, scratch=(), out=VMEM, aliases=None):
    shapes = tuple(jax.ShapeDtypeStruct(s, d) for s, d in outs)
    single = len(shapes) == 1
    return pl.pallas_call(
        kernel,
        out_shape=shapes[0] if single else shapes,
        in_specs=specs,
        out_specs=out if single else (out,) * len(shapes),
        scratch_shapes=list(scratch),
        input_output_aliases=aliases or {},
        compiler_params=pltpu.CompilerParams(vmem_limit_bytes=grant),
        cost_estimate=pl.CostEstimate(flops=flops, bytes_accessed=nbytes, transcendentals=0),
    )(*ins)


def body(entity_table, rel_phases, head_ids, rel_ids, target_pos, block_owner, block_local):
    half = rel_phases.shape[1]
    rels = rel_phases.shape[0]
    width = 2 * half
    queries = head_ids.shape[0]
    plane = lax.axis_size(PLANE)
    line = lax.axis_size(LINE)
    rows = BLK // plane
    n = 2 * BLK
    rel_rows = -(-rels // 64) * 64
    piece_rows = n * width // (plane * LANES) + rel_rows * half // 2 // (plane * LANES)

    numbers = block_owner * (entity_table.shape[0] // BLK) + block_local
    kept, passed = call(
        fetch_kernel, (numbers, entity_table), [SMEM, HBM],
        [((BLK, width), BF)] * 2, FETCH, 100_000, 500_000, [pltpu.SemaphoreType.DMA],
    )
    passed = lax.ppermute(passed, "core", SWAP)
    ids_other = lax.ppermute(rel_ids, "core", SWAP)
    block = (kept + passed).reshape(plane, rows, width)
    block = exchange(block, PLANE)
    piece = jnp.sum(block.astype(F32), axis=0).astype(BF)
    pieces = exchange(copies(piece, line), LINE).reshape(2, line // 2, rows, width)
    piece = jnp.sum(pieces.astype(F32), axis=1).astype(BF).reshape(2 * rows, width)
    own = exchange(copies(piece, plane), PLANE).reshape(n, width)
    other = lax.ppermute(own, "core", SWAP)

    heads = jnp.take(entity_table, head_ids, axis=0, mode="clip")
    cosine, sine = call(
        turn_kernel, (rel_ids, rel_phases), [SMEM, VMEM], [((queries, half), F32)] * 2,
        8 * MIB, 10_000_000, 2_000_000,
    )
    query, spot, pick, scores = call(
        early_kernel,
        (heads, cosine, sine, *(v.reshape(1, queries) for v in (target_pos, rel_ids, ids_other)), own),
        [VMEM] * 7,
        [((queries, width), BF), ((queries, LANES), jnp.int32), ((rel_rows, 2 * queries), BF),
         ((queries, n), F32)],
        12 * MIB, 4 * queries * n * width, 4_000_000,
    )

    loss, dquery, send, ang_keep, ang_send, low, rest = call(
        main_kernel, (heads, query, scores, own, other, spot, cosine, sine), [VMEM] * 8,
        [((1, queries), F32), ((queries, width), F32), ((n, width), BF),
         ((queries, half // 2), F32), ((queries, half // 2), F32),
         ((queries, n), BF), ((queries, n), BF)],
        24 * MIB, 8 * queries * n * width, 6_000_000,
    )

    got = lax.ppermute(send, "core", SWAP)
    ang_got = lax.ppermute(ang_send, "core", SWAP)
    loss, head_grad, keep, rel_keep = call(
        keep_kernel, (loss, dquery, cosine, sine, low, rest, query, own, pick, ang_keep), [VMEM] * 10,
        [((1, queries), F32), ((queries, width), BF), ((n, width), F32), ((rel_rows, half // 2), F32)],
        12 * MIB, 4 * queries * n * width, 3_000_000,
    )
    packed = call(
        pack_kernel, (pick, keep, got, rel_keep, ang_got), [VMEM] * 5,
        [((plane, piece_rows, LANES), BF)], 12 * MIB, 2 * rel_rows * queries * half, 4_000_000,
    )
    part = jnp.sum(exchange(packed, PLANE).astype(F32), axis=0).astype(BF)
    part = jnp.sum(exchange(copies(part, line), LINE).astype(F32), axis=0).astype(BF)
    own_sum = exchange(copies(part, plane), PLANE)
    other_sum = lax.ppermute(own_sum, "core", SWAP)
    shapes = [(entity_table.shape, BF), ((rels, half), F32)]
    part = pltpu.VMEM((rels, half // 2), F32)
    number = pltpu.SMEM(numbers.shape, jnp.int32)
    partial = call(
        place_own_kernel, (numbers, own_sum), [ANY, VMEM], shapes,
        8 * MIB, 1_000_000, 2_000_000,
        [pltpu.VMEM(entity_table.shape, BF), part, number, pltpu.SemaphoreType.DMA((3,))], HBM,
    )
    table_grad, rel_grad = call(
        place_other_kernel, (numbers, own_sum, other_sum, *partial),
        [ANY, VMEM, VMEM, HBM, HBM], shapes, 8 * MIB, 1_000_000, 2_000_000,
        [pltpu.VMEM((2, BLK, width), BF), pltpu.VMEM((BLK, width), F32), part, number,
         pltpu.SemaphoreType.DMA((4,))],
        HBM, {3: 0, 4: 1},
    )
    return loss.reshape(queries), head_grad, table_grad, rel_grad


def solution(mesh):
    finer = Mesh(mesh.devices.reshape(4, 4, 4, 2, mesh.shape["grp"]), ENT_GRP)
    placed = (P(ENT, None), P(), P(ENT_GRP), P(ENT_GRP), P(ENT_GRP), P(), P())
    return jax.shard_map(
        body,
        mesh=finer,
        in_specs=placed,
        out_specs=(P(ENT_GRP), P(ENT_GRP, None), P(ENT, None), P()),
        check_vma=False,
    )
```

```python
import jax
import jax.numpy as jnp
from jax import lax
from jax.experimental import pallas as pl
from jax.experimental.pallas import tpu as pltpu
from jax.sharding import Mesh
from jax.sharding import PartitionSpec as P


BLK = 128
LANES = 128
ENT = ("x", "y", "zl", "core")
ENT_GRP = ("x", "y", "zl", "core", "grp")
PLANE = ("x", "y")
LINE = ("grp", "zl")
SWAP = [(0, 1), (1, 0)]
BF = jnp.bfloat16
F32 = jnp.float32
NT = (((1,), (1,)), ((), ()))
TN = (((0,), (0,)), ((), ()))
VMEM = pl.BlockSpec(memory_space=pltpu.VMEM)
SMEM = pl.BlockSpec(memory_space=pltpu.SMEM)
ANY = pl.BlockSpec(memory_space=pl.ANY)
HBM = pl.BlockSpec(memory_space=pltpu.HBM)
MIB = 1024 * 1024
FETCH = 56_000_000


def dot(a, b, dims=(((1,), (0,)), ((), ()))):
    return lax.dot_general(a, b, dims, preferred_element_type=F32)


def halves(x):
    hi = x.astype(BF)
    return hi, (x - hi.astype(F32)).astype(BF)


def own_shard():
    place = lax.axis_index(ENT[0])
    for axis in ENT[1:]:
        place = place * lax.axis_size(axis) + lax.axis_index(axis)
    return place


def fetch_kernel(number_ref, table_ref, keep_ref, pass_ref, sems):
    core = lax.axis_index("core")
    grp = lax.axis_index("grp")
    me = own_shard()
    per = table_ref.shape[0] // BLK
    parts = sems.shape[1]
    size = BLK // parts
    waits = []
    for k, (b, out_ref) in enumerate(((2 * grp + core, keep_ref), (2 * grp + 1 - core, pass_ref))):
        mine = number_ref[b] // per == me
        start = pl.multiple_of(number_ref[b] % per * BLK, BLK)
        loads = [
            pltpu.make_async_copy(
                table_ref.at[pl.ds(start + p * size, size)],
                out_ref.at[pl.ds(p * size, size)],
                sems.at[k, p],
            )
            for p in range(parts)
        ]
        waits.append((mine, loads))

        @pl.when(mine)
        def _():
            for load in loads:
                load.start()

        @pl.when(jnp.logical_not(mine))
        def _():
            out_ref[...] = jnp.zeros_like(out_ref)

    for mine, loads in waits:

        @pl.when(mine)
        def _():
            for load in loads:
                load.wait()


def cos_sin(x):
    turns = jnp.floor(x * 0.6366197723675814 + 0.5)
    rest = ((x - turns * 1.5703125) - turns * 4.837512969970703125e-4) - turns * 7.54978995489188e-8
    z = rest * rest
    s = ((-1.9515295891e-4 * z + 8.3321608736e-3) * z - 1.6666654611e-1) * z * rest + rest
    c = ((2.443315711809948e-5 * z - 1.388731625493765e-3) * z + 4.166664568298827e-2) * z * z
    c = c - 0.5 * z + 1.0
    quarter = turns.astype(jnp.int32)
    odd = (quarter & 1) != 0
    cosine = jnp.where(odd, s, c)
    sine = jnp.where(odd, c, s)
    cosine = jnp.where(((quarter + 1) & 2) != 0, -cosine, cosine)
    sine = jnp.where((quarter & 2) != 0, -sine, sine)
    return cosine, sine


def turn_kernel(ids_ref, phases_ref, cos_ref, sin_ref):
    def take(i, carry):
        cos_ref[pl.ds(i, 1), :] = phases_ref[pl.ds(ids_ref[i], 1), :]
        return carry

    lax.fori_loop(0, cos_ref.shape[0], take, 0, unroll=16)
    cosine, sine = cos_sin(cos_ref[...])
    cos_ref[...] = cosine
    sin_ref[...] = sine


def rotated(heads_ref, cosine, sine):
    half = cosine.shape[1]
    hr = heads_ref[:, :half].astype(F32)
    hi = heads_ref[:, half:].astype(F32)
    return hr * cosine - hi * sine, hr * sine + hi * cosine


def scored(query, cand):
    wide = cand.astype(F32)
    hi, lo = halves(wide * wide)
    ones = jnp.ones((8, cand.shape[1]), BF)
    norm = (dot(ones, hi, NT) + dot(ones, lo, NT))[:1]
    return dot(query, cand, NT) - 0.5 * norm


def early_kernel(
    heads_ref, cos_ref, sin_ref, target_ref, ids_ref, ids_other_ref, own_ref,
    query_ref, spot_ref, pick_ref, scores_ref,
):
    rows, half = cos_ref.shape
    qr, qi = rotated(heads_ref, cos_ref[...], sin_ref[...])
    query_ref[:, :half] = qr.astype(BF)
    query_ref[:, half:] = qi.astype(BF)
    scores_ref[...] = scored(query_ref[...], own_ref[...])
    t = target_ref[...]
    core = lax.axis_index("core")
    block, row = t >> 7, t & 127
    spot = (((block & 1) ^ core) << 8) + ((row >> 3) << 4) + ((block >> 1) << 3) + (row & 7)
    spot_ref[...] = jnp.broadcast_to(spot, (LANES, rows)).T
    rel = lax.broadcasted_iota(jnp.int32, (pick_ref.shape[0], rows), 0)
    pick_ref[:, :rows] = (rel == ids_ref[...]).astype(F32).astype(BF)
    pick_ref[:, rows:] = (rel == ids_other_ref[...]).astype(F32).astype(BF)


def main_kernel(
    heads_ref, query_ref, scores_ref, own_ref, other_ref, spot_ref, cos_ref, sin_ref,
    loss_ref, dquery_ref, send_ref, ang_keep_ref, ang_send_ref, low_ref, rest_ref,
):
    rows, half = cos_ref.shape
    n = own_ref.shape[0]
    query = query_ref[...]
    cands = (own_ref[...], other_ref[...])
    spot = spot_ref[:, :1]
    scores = [scores_ref[...], scored(query, cands[1])]
    top = jnp.maximum(
        jnp.max(scores[0], axis=1, keepdims=True), jnp.max(scores[1], axis=1, keepdims=True)
    )
    exps = [jnp.exp(s - top) for s in scores]
    total = jnp.sum(exps[0], axis=1, keepdims=True) + jnp.sum(exps[1], axis=1, keepdims=True)
    lanes = lax.broadcasted_iota(jnp.int32, (rows, n), 1)
    hits = [lanes == spot, lanes + n == spot]
    picked = sum(jnp.sum(jnp.where(h, s, 0.0), axis=1, keepdims=True) for h, s in zip(hits, scores))
    loss = top + jnp.log(total) - picked
    loss_ref[...] = jnp.broadcast_to(loss, (rows, LANES)).T[:1]
    scale = 1.0 / total
    dquery = None
    for k in (1, 0):
        weights = exps[k] * scale - hits[k].astype(F32)
        low, rest = halves(weights)
        part = dot(low, cands[k])
        dquery = part if dquery is None else dquery + part
        if k == 0:
            low_ref[...] = low
            rest_ref[...] = rest
        else:
            send_ref[...] = pulled(low, rest, query, cands[k]).astype(BF)
    cosine = cos_ref[...]
    sine = sin_ref[...]
    qr, qi = rotated(heads_ref, cosine, sine)
    dr, di = dquery[:, :half], dquery[:, half:]
    dquery_ref[...] = dquery
    ang = di * qr - dr * qi
    a, b = ang[:, : half // 2], ang[:, half // 2 :]
    first = lax.axis_index("core") == 0
    ang_keep_ref[...] = jnp.where(first, a, b)
    ang_send_ref[...] = jnp.where(first, b, a)


def pulled(low, rest, query, cand):
    ones = jnp.ones((low.shape[0], LANES), BF)
    column = (dot(low, ones, TN) + dot(rest, ones, TN))[:, :1]
    return dot(low, query, TN) - column * cand.astype(F32)


def keep_kernel(
    loss_in_ref, dquery_ref, cos_ref, sin_ref, low_ref, rest_ref, query_ref, own_ref, pick_ref, ang_ref,
    loss_ref, head_ref, keep_ref, rel_ref,
):
    half = cos_ref.shape[1]
    loss_ref[...] = loss_in_ref[...]
    cosine = cos_ref[...]
    sine = sin_ref[...]
    dr, di = dquery_ref[:, :half], dquery_ref[:, half:]
    head_ref[:, :half] = (dr * cosine + di * sine).astype(BF)
    head_ref[:, half:] = (di * cosine - dr * sine).astype(BF)
    keep_ref[...] = pulled(low_ref[...], rest_ref[...], query_ref[...], own_ref[...])
    hi, lo = halves(ang_ref[...])
    sel = pick_ref[:, : ang_ref.shape[0]]
    rel_ref[...] = dot(sel, hi) + dot(sel, lo)


def pack_kernel(pick_ref, keep_ref, got_ref, rel_ref, ang_got_ref, out_ref):
    pieces = out_ref.shape[0]
    per = keep_ref.shape[0] // pieces
    groups = keep_ref.shape[1] // LANES
    for k in range(groups):
        cols = slice(k * LANES, (k + 1) * LANES)
        grad = keep_ref[:, cols] + got_ref[:, cols].astype(F32)
        out_ref[:, k * per : (k + 1) * per, :] = grad.astype(BF).reshape(pieces, per, LANES)
    hi, lo = halves(ang_got_ref[...])
    sel = pick_ref[:, ang_got_ref.shape[0] :]
    total = (rel_ref[...] + (dot(sel, hi) + dot(sel, lo))).astype(BF)
    base = groups * per
    size = out_ref.shape[1] - base
    row_groups = total.shape[0] // size
    for j in range(pieces):
        at = (j % row_groups) * size
        col = (j // row_groups) * LANES
        out_ref[j, base:, :] = total[at : at + size, col : col + LANES]


def block_of(src_ref, g, k):
    per = BLK // src_ref.shape[0]
    at = (k * 2 + g) * per
    return src_ref[:, at : at + per, :].astype(F32).reshape(BLK, LANES)


def spread(src_ref, part_ref):
    pieces, piece_rows, _ = src_ref.shape
    row_groups = pieces * LANES // part_ref.shape[1]
    base = 2 * BLK * 8 // pieces
    size = piece_rows - base
    for j in range(pieces):
        at = (j % row_groups) * size
        rows = min(size, part_ref.shape[0] - at)
        col = (j // row_groups) * LANES
        part_ref[at : at + rows, col : col + LANES] = src_ref[j, base : base + rows, :].astype(F32)


def half_columns(rel_ref, part_ref, half):
    w = part_ref.shape[1]
    return rel_ref.at[:, pl.ds(pl.multiple_of(half * w, w), w)]


def place_own_kernel(
    numbers_ref, own_ref, table_ref, rel_ref, rows_ref, part_ref, number_ref, sems
):
    core = lax.axis_index("core")
    me = own_shard()
    per = table_ref.shape[0] // BLK
    load = pltpu.make_async_copy(numbers_ref, number_ref, sems.at[2])
    load.start()
    spread(own_ref, part_ref)
    part = pltpu.make_async_copy(part_ref, half_columns(rel_ref, part_ref, core), sems.at[1])
    part.start()
    rows_ref[...] = jnp.zeros_like(rows_ref)
    load.wait()
    for g in range(2):
        b = 2 * g + core

        @pl.when(number_ref[b] // per == me)
        def _():
            at = pl.ds(pl.multiple_of(number_ref[b] % per * BLK, BLK), BLK)
            for k in range(rows_ref.shape[1] // LANES):
                cols = slice(k * LANES, (k + 1) * LANES)
                old = rows_ref[at, cols].astype(F32)
                rows_ref[at, cols] = (old + block_of(own_ref, g, k)).astype(BF)

    table = pltpu.make_async_copy(rows_ref, table_ref, sems.at[0])
    table.start()
    table.wait()
    part.wait()


def place_other_kernel(
    numbers_ref, own_ref, other_ref, table_in_ref, rel_in_ref,
    table_ref, rel_ref, rows_ref, sum_ref, part_ref, number_ref, sems,
):
    del table_in_ref, rel_in_ref
    core = lax.axis_index("core")
    me = own_shard()
    per = table_ref.shape[0] // BLK
    groups = rows_ref.shape[2] // LANES
    load = pltpu.make_async_copy(numbers_ref, number_ref, sems.at[3])
    load.start()
    spread(other_ref, part_ref)
    part = pltpu.make_async_copy(part_ref, half_columns(rel_ref, part_ref, 1 - core), sems.at[2])
    part.start()
    load.wait()
    blocks = []
    for g in range(2):
        b = 2 * g + 1 - core
        at = pl.ds(pl.multiple_of(number_ref[b] % per * BLK, BLK), BLK)
        copy = pltpu.make_async_copy(rows_ref.at[g], table_ref.at[at], sems.at[g])
        mine = number_ref[b] // per == me
        if g == 1:
            mine = mine & (number_ref[b] != number_ref[1 - core])
        blocks.append((mine, copy))

        @pl.when(mine)
        def _():
            for k in range(groups):
                cols = slice(k * LANES, (k + 1) * LANES)
                sum_ref[:, cols] = block_of(other_ref, g, k)
            twins = ((own_ref, core, 0), (own_ref, 2 + core, 1), (other_ref, 2 * (1 - g) + 1 - core, 1 - g))
            for src_ref, c, h in twins:

                @pl.when(number_ref[c] == number_ref[b])
                def _():
                    for k in range(groups):
                        cols = slice(k * LANES, (k + 1) * LANES)
                        sum_ref[:, cols] = sum_ref[:, cols] + block_of(src_ref, h, k)

            rows_ref[g] = sum_ref[...].astype(BF)
            copy.start()

    for mine, copy in blocks:
        pl.when(mine)(copy.wait)
    part.wait()


def exchange(x, axes):
    return lax.all_to_all(x, axes, split_axis=0, concat_axis=0, tiled=True)


def copies(x, n):
    return jnp.broadcast_to(x[None], (n, *x.shape))


def call(kernel, ins, specs, outs, grant, flops, nbytes, scratch=(), out=VMEM, aliases=None):
    shapes = tuple(jax.ShapeDtypeStruct(s, d) for s, d in outs)
    single = len(shapes) == 1
    return pl.pallas_call(
        kernel,
        out_shape=shapes[0] if single else shapes,
        in_specs=specs,
        out_specs=out if single else (out,) * len(shapes),
        scratch_shapes=list(scratch),
        input_output_aliases=aliases or {},
        compiler_params=pltpu.CompilerParams(vmem_limit_bytes=grant),
        cost_estimate=pl.CostEstimate(flops=flops, bytes_accessed=nbytes, transcendentals=0),
    )(*ins)


def body(entity_table, rel_phases, head_ids, rel_ids, target_pos, block_owner, block_local):
    half = rel_phases.shape[1]
    rels = rel_phases.shape[0]
    width = 2 * half
    queries = head_ids.shape[0]
    plane = lax.axis_size(PLANE)
    line = lax.axis_size(LINE)
    rows = BLK // plane
    n = 2 * BLK
    rel_rows = -(-rels // 64) * 64
    piece_rows = n * width // (plane * LANES) + rel_rows * half // 2 // (plane * LANES)

    numbers = block_owner * (entity_table.shape[0] // BLK) + block_local
    kept, passed = call(
        fetch_kernel, (numbers, entity_table), [SMEM, HBM],
        [((BLK, width), BF)] * 2, FETCH, 100_000, 500_000, [pltpu.SemaphoreType.DMA((2, 4))],
    )
    passed = lax.ppermute(passed, "core", SWAP)
    ids_other = lax.ppermute(rel_ids, "core", SWAP)
    block = (kept + passed).reshape(plane, rows, width)
    block = exchange(block, PLANE)
    piece = jnp.sum(block.astype(F32), axis=0).astype(BF)
    pieces = exchange(copies(piece, line), LINE).reshape(2, line // 2, rows, width)
    piece = jnp.sum(pieces.astype(F32), axis=1).astype(BF).reshape(2 * rows, width)
    own = exchange(copies(piece, plane), PLANE).reshape(n, width)
    other = lax.ppermute(own, "core", SWAP)

    heads = jnp.take(entity_table, head_ids, axis=0, mode="clip")
    cosine, sine = call(
        turn_kernel, (rel_ids, rel_phases), [SMEM, VMEM], [((queries, half), F32)] * 2,
        8 * MIB, 10_000_000, 2_000_000,
    )
    query, spot, pick, scores = call(
        early_kernel,
        (heads, cosine, sine, *(v.reshape(1, queries) for v in (target_pos, rel_ids, ids_other)), own),
        [VMEM] * 7,
        [((queries, width), BF), ((queries, LANES), jnp.int32), ((rel_rows, 2 * queries), BF),
         ((queries, n), F32)],
        12 * MIB, 4 * queries * n * width, 4_000_000,
    )

    loss, dquery, send, ang_keep, ang_send, low, rest = call(
        main_kernel, (heads, query, scores, own, other, spot, cosine, sine), [VMEM] * 8,
        [((1, queries), F32), ((queries, width), F32), ((n, width), BF),
         ((queries, half // 2), F32), ((queries, half // 2), F32),
         ((queries, n), BF), ((queries, n), BF)],
        24 * MIB, 8 * queries * n * width, 6_000_000,
    )

    got = lax.ppermute(send, "core", SWAP)
    ang_got = lax.ppermute(ang_send, "core", SWAP)
    loss, head_grad, keep, rel_keep = call(
        keep_kernel, (loss, dquery, cosine, sine, low, rest, query, own, pick, ang_keep), [VMEM] * 10,
        [((1, queries), F32), ((queries, width), BF), ((n, width), F32), ((rel_rows, half // 2), F32)],
        12 * MIB, 4 * queries * n * width, 3_000_000,
    )
    packed = call(
        pack_kernel, (pick, keep, got, rel_keep, ang_got), [VMEM] * 5,
        [((plane, piece_rows, LANES), BF)], 12 * MIB, 2 * rel_rows * queries * half, 4_000_000,
    )
    part = jnp.sum(exchange(packed, PLANE).astype(F32), axis=0).astype(BF)
    part = jnp.sum(exchange(copies(part, line), LINE).astype(F32), axis=0).astype(BF)
    own_sum = exchange(copies(part, plane), PLANE)
    other_sum = lax.ppermute(own_sum, "core", SWAP)
    shapes = [(entity_table.shape, BF), ((rels, half), F32)]
    part = pltpu.VMEM((rels, half // 2), F32)
    number = pltpu.SMEM(numbers.shape, jnp.int32)
    partial = call(
        place_own_kernel, (numbers, own_sum), [ANY, VMEM], shapes,
        8 * MIB, 1_000_000, 2_000_000,
        [pltpu.VMEM(entity_table.shape, BF), part, number, pltpu.SemaphoreType.DMA((3,))], HBM,
    )
    table_grad, rel_grad = call(
        place_other_kernel, (numbers, own_sum, other_sum, *partial),
        [ANY, VMEM, VMEM, HBM, HBM], shapes, 8 * MIB, 1_000_000, 2_000_000,
        [pltpu.VMEM((2, BLK, width), BF), pltpu.VMEM((BLK, width), F32), part, number,
         pltpu.SemaphoreType.DMA((4,))],
        HBM, {3: 0, 4: 1},
    )
    return loss.reshape(queries), head_grad, table_grad, rel_grad


def solution(mesh):
    finer = Mesh(mesh.devices.reshape(4, 4, 4, 2, mesh.shape["grp"]), ENT_GRP)
    placed = (P(ENT, None), P(), P(ENT_GRP), P(ENT_GRP), P(ENT_GRP), P(), P())
    return jax.shard_map(
        body,
        mesh=finer,
        in_specs=placed,
        out_specs=(P(ENT_GRP), P(ENT_GRP, None), P(ENT, None), P()),
        check_vma=False,
    )
```

```python
import jax
import jax.numpy as jnp
from jax import lax
from jax.experimental import pallas as pl
from jax.experimental.pallas import tpu as pltpu
from jax.sharding import Mesh
from jax.sharding import PartitionSpec as P


BLK = 128
LANES = 128
ENT = ("x", "y", "zl", "core")
ENT_GRP = ("x", "y", "zl", "core", "grp")
PLANE = ("x", "y")
LINE = ("grp", "zl")
SWAP = [(0, 1), (1, 0)]
BF = jnp.bfloat16
F32 = jnp.float32
NT = (((1,), (1,)), ((), ()))
TN = (((0,), (0,)), ((), ()))
VMEM = pl.BlockSpec(memory_space=pltpu.VMEM)
SMEM = pl.BlockSpec(memory_space=pltpu.SMEM)
ANY = pl.BlockSpec(memory_space=pl.ANY)
HBM = pl.BlockSpec(memory_space=pltpu.HBM)
MIB = 1024 * 1024
FETCH = 56_000_000


def dot(a, b, dims=(((1,), (0,)), ((), ()))):
    return lax.dot_general(a, b, dims, preferred_element_type=F32)


def halves(x):
    hi = x.astype(BF)
    return hi, (x - hi.astype(F32)).astype(BF)


def own_shard():
    place = lax.axis_index(ENT[0])
    for axis in ENT[1:]:
        place = place * lax.axis_size(axis) + lax.axis_index(axis)
    return place


def fetch_kernel(number_ref, table_ref, keep_ref, pass_ref, sem):
    core = lax.axis_index("core")
    grp = lax.axis_index("grp")
    me = own_shard()
    per = table_ref.shape[0] // BLK
    for b, out_ref in ((2 * grp + core, keep_ref), (2 * grp + 1 - core, pass_ref)):

        @pl.when(number_ref[b] // per == me)
        def _():
            start = pl.multiple_of(number_ref[b] % per * BLK, BLK)
            copy = pltpu.make_async_copy(table_ref.at[pl.ds(start, BLK)], out_ref, sem)
            copy.start()
            copy.wait()

        @pl.when(number_ref[b] // per != me)
        def _():
            out_ref[...] = jnp.zeros_like(out_ref)


def cos_sin(x):
    turns = jnp.floor(x * 0.6366197723675814 + 0.5)
    rest = ((x - turns * 1.5703125) - turns * 4.837512969970703125e-4) - turns * 7.54978995489188e-8
    z = rest * rest
    s = ((-1.9515295891e-4 * z + 8.3321608736e-3) * z - 1.6666654611e-1) * z * rest + rest
    c = ((2.443315711809948e-5 * z - 1.388731625493765e-3) * z + 4.166664568298827e-2) * z * z
    c = c - 0.5 * z + 1.0
    quarter = turns.astype(jnp.int32)
    odd = (quarter & 1) != 0
    cosine = jnp.where(odd, s, c)
    sine = jnp.where(odd, c, s)
    cosine = jnp.where(((quarter + 1) & 2) != 0, -cosine, cosine)
    sine = jnp.where((quarter & 2) != 0, -sine, sine)
    return cosine, sine


def turn_kernel(ids_ref, phases_ref, cos_ref, sin_ref):
    def take(i, carry):
        cos_ref[pl.ds(i, 1), :] = phases_ref[pl.ds(ids_ref[i], 1), :]
        return carry

    lax.fori_loop(0, cos_ref.shape[0], take, 0, unroll=16)
    cosine, sine = cos_sin(cos_ref[...])
    cos_ref[...] = cosine
    sin_ref[...] = sine


def rotated(heads_ref, cosine, sine):
    half = cosine.shape[1]
    hr = heads_ref[:, :half].astype(F32)
    hi = heads_ref[:, half:].astype(F32)
    return hr * cosine - hi * sine, hr * sine + hi * cosine


def scored(query, cand):
    wide = cand.astype(F32)
    hi, lo = halves(wide * wide)
    ones = jnp.ones((8, cand.shape[1]), BF)
    norm = (dot(ones, hi, NT) + dot(ones, lo, NT))[:1]
    return dot(query, cand, NT) - 0.5 * norm


def early_kernel(
    heads_ref, cos_ref, sin_ref, target_ref, ids_ref, ids_other_ref, own_ref,
    query_ref, spot_ref, pick_ref, scores_ref,
):
    rows, half = cos_ref.shape
    qr, qi = rotated(heads_ref, cos_ref[...], sin_ref[...])
    query_ref[:, :half] = qr.astype(BF)
    query_ref[:, half:] = qi.astype(BF)
    scores_ref[...] = scored(query_ref[...], own_ref[...])
    t = target_ref[...]
    core = lax.axis_index("core")
    block, row = t >> 7, t & 127
    spot = (((block & 1) ^ core) << 8) + ((row >> 3) << 4) + ((block >> 1) << 3) + (row & 7)
    spot_ref[...] = jnp.broadcast_to(spot, (LANES, rows)).T
    rel = lax.broadcasted_iota(jnp.int32, (pick_ref.shape[0], rows), 0)
    pick_ref[:, :rows] = (rel == ids_ref[...]).astype(F32).astype(BF)
    pick_ref[:, rows:] = (rel == ids_other_ref[...]).astype(F32).astype(BF)


def main_kernel(
    heads_ref, query_ref, scores_ref, own_ref, other_ref, spot_ref, cos_ref, sin_ref,
    loss_ref, dquery_ref, send_ref, ang_keep_ref, low_ref, rest_ref,
):
    rows, half = cos_ref.shape
    n = own_ref.shape[0]
    query = query_ref[...]
    cands = (own_ref[...], other_ref[...])
    spot = spot_ref[:, :1]
    scores = [scores_ref[...], scored(query, cands[1])]
    top = jnp.maximum(
        jnp.max(scores[0], axis=1, keepdims=True), jnp.max(scores[1], axis=1, keepdims=True)
    )
    exps = [jnp.exp(s - top) for s in scores]
    total = jnp.sum(exps[0], axis=1, keepdims=True) + jnp.sum(exps[1], axis=1, keepdims=True)
    lanes = lax.broadcasted_iota(jnp.int32, (rows, n), 1)
    hits = [lanes == spot, lanes + n == spot]
    picked = sum(jnp.sum(jnp.where(h, s, 0.0), axis=1, keepdims=True) for h, s in zip(hits, scores))
    loss = top + jnp.log(total) - picked
    loss_ref[...] = jnp.broadcast_to(loss, (rows, LANES)).T[:1]
    scale = 1.0 / total
    dquery = None
    for k in (1, 0):
        weights = exps[k] * scale - hits[k].astype(F32)
        low, rest = halves(weights)
        part = dot(low, cands[k])
        dquery = part if dquery is None else dquery + part
        if k == 0:
            low_ref[...] = low
            rest_ref[...] = rest
        else:
            send_ref[:, : 2 * half] = pulled(low, rest, query, cands[k]).astype(BF)
    cosine = cos_ref[...]
    sine = sin_ref[...]
    qr, qi = rotated(heads_ref, cosine, sine)
    dr, di = dquery[:, :half], dquery[:, half:]
    dquery_ref[...] = dquery
    ang = di * qr - dr * qi
    a, b = ang[:, : half // 2], ang[:, half // 2 :]
    first = lax.axis_index("core") == 0
    ang_keep_ref[...] = jnp.where(first, a, b)
    hi, lo = halves(jnp.where(first, b, a))
    send_ref[:, 2 * half : 2 * half + half // 2] = hi
    send_ref[:, 2 * half + half // 2 :] = lo


def pulled(low, rest, query, cand):
    ones = jnp.ones((low.shape[0], LANES), BF)
    column = (dot(low, ones, TN) + dot(rest, ones, TN))[:, :1]
    return dot(low, query, TN) - column * cand.astype(F32)


def keep_kernel(
    loss_in_ref, dquery_ref, cos_ref, sin_ref, low_ref, rest_ref, query_ref, own_ref, pick_ref, ang_ref,
    loss_ref, head_ref, keep_ref, rel_ref,
):
    half = cos_ref.shape[1]
    loss_ref[...] = loss_in_ref[...]
    cosine = cos_ref[...]
    sine = sin_ref[...]
    dr, di = dquery_ref[:, :half], dquery_ref[:, half:]
    head_ref[:, :half] = (dr * cosine + di * sine).astype(BF)
    head_ref[:, half:] = (di * cosine - dr * sine).astype(BF)
    keep_ref[...] = pulled(low_ref[...], rest_ref[...], query_ref[...], own_ref[...])
    hi, lo = halves(ang_ref[...])
    sel = pick_ref[:, : ang_ref.shape[0]]
    rel_ref[...] = dot(sel, hi) + dot(sel, lo)


def pack_kernel(pick_ref, keep_ref, got_ref, rel_ref, out_ref):
    pieces = out_ref.shape[0]
    per = keep_ref.shape[0] // pieces
    groups = keep_ref.shape[1] // LANES
    for k in range(groups):
        cols = slice(k * LANES, (k + 1) * LANES)
        grad = keep_ref[:, cols] + got_ref[:, cols].astype(F32)
        out_ref[:, k * per : (k + 1) * per, :] = grad.astype(BF).reshape(pieces, per, LANES)
    w = keep_ref.shape[1]
    hi = got_ref[:, w : w + w // 4]
    lo = got_ref[:, w + w // 4 :]
    sel = pick_ref[:, got_ref.shape[0] :]
    total = (rel_ref[...] + (dot(sel, hi) + dot(sel, lo))).astype(BF)
    base = groups * per
    size = out_ref.shape[1] - base
    row_groups = total.shape[0] // size
    for j in range(pieces):
        at = (j % row_groups) * size
        col = (j // row_groups) * LANES
        out_ref[j, base:, :] = total[at : at + size, col : col + LANES]


def block_of(src_ref, g, k):
    per = BLK // src_ref.shape[0]
    at = (k * 2 + g) * per
    return src_ref[:, at : at + per, :].astype(F32).reshape(BLK, LANES)


def spread(src_ref, part_ref):
    pieces, piece_rows, _ = src_ref.shape
    row_groups = pieces * LANES // part_ref.shape[1]
    base = 2 * BLK * 8 // pieces
    size = piece_rows - base
    for j in range(pieces):
        at = (j % row_groups) * size
        rows = min(size, part_ref.shape[0] - at)
        col = (j // row_groups) * LANES
        part_ref[at : at + rows, col : col + LANES] = src_ref[j, base : base + rows, :].astype(F32)


def half_columns(rel_ref, part_ref, half):
    w = part_ref.shape[1]
    return rel_ref.at[:, pl.ds(pl.multiple_of(half * w, w), w)]


def place_own_kernel(
    numbers_ref, own_ref, table_ref, rel_ref, rows_ref, part_ref, number_ref, sems
):
    core = lax.axis_index("core")
    me = own_shard()
    per = table_ref.shape[0] // BLK
    load = pltpu.make_async_copy(numbers_ref, number_ref, sems.at[2])
    load.start()
    spread(own_ref, part_ref)
    part = pltpu.make_async_copy(part_ref, half_columns(rel_ref, part_ref, core), sems.at[1])
    part.start()
    rows_ref[...] = jnp.zeros_like(rows_ref)
    load.wait()
    for g in range(2):
        b = 2 * g + core

        @pl.when(number_ref[b] // per == me)
        def _():
            at = pl.ds(pl.multiple_of(number_ref[b] % per * BLK, BLK), BLK)
            for k in range(rows_ref.shape[1] // LANES):
                cols = slice(k * LANES, (k + 1) * LANES)
                old = rows_ref[at, cols].astype(F32)
                rows_ref[at, cols] = (old + block_of(own_ref, g, k)).astype(BF)

    table = pltpu.make_async_copy(rows_ref, table_ref, sems.at[0])
    table.start()
    table.wait()
    part.wait()


def place_other_kernel(
    numbers_ref, own_ref, other_ref, table_in_ref, rel_in_ref,
    table_ref, rel_ref, rows_ref, sum_ref, part_ref, number_ref, sems,
):
    del table_in_ref, rel_in_ref
    core = lax.axis_index("core")
    me = own_shard()
    per = table_ref.shape[0] // BLK
    groups = rows_ref.shape[2] // LANES
    load = pltpu.make_async_copy(numbers_ref, number_ref, sems.at[3])
    load.start()
    spread(other_ref, part_ref)
    part = pltpu.make_async_copy(part_ref, half_columns(rel_ref, part_ref, 1 - core), sems.at[2])
    part.start()
    load.wait()
    blocks = []
    for g in range(2):
        b = 2 * g + 1 - core
        at = pl.ds(pl.multiple_of(number_ref[b] % per * BLK, BLK), BLK)
        copy = pltpu.make_async_copy(rows_ref.at[g], table_ref.at[at], sems.at[g])
        mine = number_ref[b] // per == me
        if g == 1:
            mine = mine & (number_ref[b] != number_ref[1 - core])
        blocks.append((mine, copy))

        @pl.when(mine)
        def _():
            for k in range(groups):
                cols = slice(k * LANES, (k + 1) * LANES)
                sum_ref[:, cols] = block_of(other_ref, g, k)
            twins = ((own_ref, core, 0), (own_ref, 2 + core, 1), (other_ref, 2 * (1 - g) + 1 - core, 1 - g))
            for src_ref, c, h in twins:

                @pl.when(number_ref[c] == number_ref[b])
                def _():
                    for k in range(groups):
                        cols = slice(k * LANES, (k + 1) * LANES)
                        sum_ref[:, cols] = sum_ref[:, cols] + block_of(src_ref, h, k)

            rows_ref[g] = sum_ref[...].astype(BF)
            copy.start()

    for mine, copy in blocks:
        pl.when(mine)(copy.wait)
    part.wait()


def exchange(x, axes):
    return lax.all_to_all(x, axes, split_axis=0, concat_axis=0, tiled=True)


def copies(x, n):
    return jnp.broadcast_to(x[None], (n, *x.shape))


def call(kernel, ins, specs, outs, grant, flops, nbytes, scratch=(), out=VMEM, aliases=None):
    shapes = tuple(jax.ShapeDtypeStruct(s, d) for s, d in outs)
    single = len(shapes) == 1
    return pl.pallas_call(
        kernel,
        out_shape=shapes[0] if single else shapes,
        in_specs=specs,
        out_specs=out if single else (out,) * len(shapes),
        scratch_shapes=list(scratch),
        input_output_aliases=aliases or {},
        compiler_params=pltpu.CompilerParams(vmem_limit_bytes=grant),
        cost_estimate=pl.CostEstimate(flops=flops, bytes_accessed=nbytes, transcendentals=0),
    )(*ins)


def body(entity_table, rel_phases, head_ids, rel_ids, target_pos, block_owner, block_local):
    half = rel_phases.shape[1]
    rels = rel_phases.shape[0]
    width = 2 * half
    queries = head_ids.shape[0]
    plane = lax.axis_size(PLANE)
    line = lax.axis_size(LINE)
    rows = BLK // plane
    n = 2 * BLK
    rel_rows = -(-rels // 64) * 64
    piece_rows = n * width // (plane * LANES) + rel_rows * half // 2 // (plane * LANES)

    numbers = block_owner * (entity_table.shape[0] // BLK) + block_local
    kept, passed = call(
        fetch_kernel, (numbers, entity_table), [SMEM, HBM],
        [((BLK, width), BF)] * 2, FETCH, 100_000, 500_000, [pltpu.SemaphoreType.DMA],
    )
    passed = lax.ppermute(passed, "core", SWAP)
    ids_other = lax.ppermute(rel_ids, "core", SWAP)
    block = (kept + passed).reshape(plane, rows, width)
    block = exchange(block, PLANE)
    piece = jnp.sum(block.astype(F32), axis=0).astype(BF)
    pieces = exchange(copies(piece, line), LINE).reshape(2, line // 2, rows, width)
    piece = jnp.sum(pieces.astype(F32), axis=1).astype(BF).reshape(2 * rows, width)
    own = exchange(copies(piece, plane), PLANE).reshape(n, width)
    other = lax.ppermute(own, "core", SWAP)

    heads = jnp.take(entity_table, head_ids, axis=0, mode="clip")
    cosine, sine = call(
        turn_kernel, (rel_ids, rel_phases), [SMEM, VMEM], [((queries, half), F32)] * 2,
        8 * MIB, 10_000_000, 2_000_000,
    )
    query, spot, pick, scores = call(
        early_kernel,
        (heads, cosine, sine, *(v.reshape(1, queries) for v in (target_pos, rel_ids, ids_other)), own),
        [VMEM] * 7,
        [((queries, width), BF), ((queries, LANES), jnp.int32), ((rel_rows, 2 * queries), BF),
         ((queries, n), F32)],
        12 * MIB, 4 * queries * n * width, 4_000_000,
    )

    loss, dquery, send, ang_keep, low, rest = call(
        main_kernel, (heads, query, scores, own, other, spot, cosine, sine), [VMEM] * 8,
        [((1, queries), F32), ((queries, width), F32), ((n, width + half), BF),
         ((queries, half // 2), F32),
         ((queries, n), BF), ((queries, n), BF)],
        24 * MIB, 8 * queries * n * width, 6_000_000,
    )

    got = lax.ppermute(send, "core", SWAP)
    loss, head_grad, keep, rel_keep = call(
        keep_kernel, (loss, dquery, cosine, sine, low, rest, query, own, pick, ang_keep), [VMEM] * 10,
        [((1, queries), F32), ((queries, width), BF), ((n, width), F32), ((rel_rows, half // 2), F32)],
        12 * MIB, 4 * queries * n * width, 3_000_000,
    )
    packed = call(
        pack_kernel, (pick, keep, got, rel_keep), [VMEM] * 4,
        [((plane, piece_rows, LANES), BF)], 12 * MIB, 2 * rel_rows * queries * half, 4_000_000,
    )
    part = jnp.sum(exchange(packed, PLANE).astype(F32), axis=0).astype(BF)
    part = jnp.sum(exchange(copies(part, line), LINE).astype(F32), axis=0).astype(BF)
    own_sum = exchange(copies(part, plane), PLANE)
    other_sum = lax.ppermute(own_sum, "core", SWAP)
    shapes = [(entity_table.shape, BF), ((rels, half), F32)]
    part = pltpu.VMEM((rels, half // 2), F32)
    number = pltpu.SMEM(numbers.shape, jnp.int32)
    partial = call(
        place_own_kernel, (numbers, own_sum), [ANY, VMEM], shapes,
        8 * MIB, 1_000_000, 2_000_000,
        [pltpu.VMEM(entity_table.shape, BF), part, number, pltpu.SemaphoreType.DMA((3,))], HBM,
    )
    table_grad, rel_grad = call(
        place_other_kernel, (numbers, own_sum, other_sum, *partial),
        [ANY, VMEM, VMEM, HBM, HBM], shapes, 8 * MIB, 1_000_000, 2_000_000,
        [pltpu.VMEM((2, BLK, width), BF), pltpu.VMEM((BLK, width), F32), part, number,
         pltpu.SemaphoreType.DMA((4,))],
        HBM, {3: 0, 4: 1},
    )
    return loss.reshape(queries), head_grad, table_grad, rel_grad


def solution(mesh):
    finer = Mesh(mesh.devices.reshape(4, 4, 4, 2, mesh.shape["grp"]), ENT_GRP)
    placed = (P(ENT, None), P(), P(ENT_GRP), P(ENT_GRP), P(ENT_GRP), P(), P())
    return jax.shard_map(
        body,
        mesh=finer,
        in_specs=placed,
        out_specs=(P(ENT_GRP), P(ENT_GRP, None), P(ENT, None), P()),
        check_vma=False,
    )
```
